32 devices in a mesh: dp: 8 (over z, x), tp: 4 (over y, core).
Axes of the slice: x: 2, y: 2, z: 4, core: 2. Of those that a mesh axis runs over, the one named last changes fastest.
Arguments:
- hidden_in: bfloat16 [512, 3584], P(('dp', 'tp')), may hold values from -6 to 6
- query_latent: bfloat16 [512, 64, 512], P(('dp', 'tp')), may hold values from -348 to 347
- query_rope: bfloat16 [512, 4096], P(('dp', 'tp')), may hold values from -348 to 347
- cache_latent: bfloat16 [512, 128, 512], P(('dp', 'tp')), may hold values from -6 to 6
- cache_rope: bfloat16 [512, 64, 128], P(('dp', 'tp')), may hold values from -6 to 6
- lengths: int32 [512], P(('dp', 'tp')), may hold values from 16 to 128
- value_up: bfloat16 [512, 4096], P(None, 'tp'), may hold values from -1 to 1
- out_proj: bfloat16 [4096, 3584], P('tp'), may hold values from -0.09375 to 0.09375
- norm_gain: float32 [3584], replicated, may hold values from 0.1 to 1.9
- expert_gate: bfloat16 [32, 3584, 1024], P(('dp', 'tp')), may hold values from -0.09375 to 0.09375
- expert_down: bfloat16 [32, 1024, 3584], P(('dp', 'tp')), may hold values from -0.1875 to 0.1875
- expert_ids: int32 [512, 8], P(('dp', 'tp')), may hold values from 0 to 31, all different within a row; in each aligned block of 16 rows (0 to 15, 16 to 31, ...) at most 4 rows name the same one
- affinity: float32 [512, 8], P(('dp', 'tp')), may hold values from 0.05 to 1
Outputs:
- layer_out: bfloat16 [512, 3584], P(('dp', 'tp'))
The draws below stay inside these ranges and needn't reach their ends.
Inputs may be any that keep to these rules, and one draw needn't show every extreme that they name: `expert_ids`: in each aligned block of 16 rows (the rows of one device) no expert is named by more than 4 rows.
All inputs are finite; a program needn't handle non-finite values.
Results may differ from the reference program's by a relative error of at most 0.0081.
Values may be sent and summed in bfloat16 or wider, within the bound.
A program may use at most 128 MiB of HBM per device.

```python
import math
import jax
import jax.numpy as jnp
import numpy as np
from jax import lax

D = 3584
HEADS = 64
LAT = 512
ROPE = 64
HEAD_V = 64
FF = 1024
TOPK = 8
CTX = 128
TOK_DEV = 16
TOKENS = 512
EXPERTS = 32
CAP = 4


def key_parts(key):
    latent = jax.random.normal(jax.random.fold_in(key, 101), (TOKENS, CTX, LAT), jnp.float32)
    rotary = jax.random.normal(jax.random.fold_in(key, 102), (TOKENS, ROPE, CTX), jnp.float32)
    latent = jnp.clip(latent, -6.0, 6.0).astype(jnp.bfloat16).astype(jnp.float32)
    rotary = jnp.clip(rotary, -6.0, 6.0).astype(jnp.bfloat16).astype(jnp.float32)
    return (latent, rotary)


def draw_cache_latent(key, part):
    return key_parts(key)[0].astype(jnp.bfloat16)


def draw_cache_rope(key, part):
    return key_parts(key)[1].astype(jnp.bfloat16)


def query_parts(key):
    full_shape = (TOKENS, HEADS, LAT + ROPE)
    return jnp.clip(jax.random.normal(jax.random.fold_in(key, 103), full_shape, jnp.float32), -6.0, 6.0)


def draw_query_latent(key, part):
    return query_parts(key)[:, :, :LAT].astype(jnp.bfloat16)


def draw_query_rope(key, part):
    return query_parts(key)[:, :, LAT:].reshape(TOKENS, HEADS * ROPE).astype(jnp.bfloat16)


def plant(result, rng, smallest, high):
    spot = [jax.random.randint(jax.random.fold_in(rng, axis), (), 0, length) for axis, length in enumerate(result.shape)]
    main_axis = result.shape.index(max(result.shape))
    beside = spot[:main_axis] + [(spot[main_axis] + 1) % result.shape[main_axis]] + spot[main_axis + 1:]
    return result.at[tuple(spot)].set(smallest).at[tuple(beside)].set(high)


def shard_levels(own_key, extent, pieces, smallest, top_value):
    def one(axis_at, shards_of):
        draws = jax.random.uniform(jax.random.fold_in(jax.random.fold_in(own_key, 6), axis_at), (shards_of,), jnp.float32, smallest / len(pieces), top_value / len(pieces))
        return jnp.repeat(jnp.exp(draws), extent[axis_at] // shards_of).reshape((-1,) + (1,) * (len(extent) - axis_at - 1))

    level = one(*pieces[0])
    for cut in pieces[1:]:
        level = level * one(*cut)
    return level


def shared_out(key, own, number, rows, number_of, top, limit, slope):
    sequence = jax.random.permutation(key, number_of)
    heavy_load, common = load_shares(number_of, rows * top, limit, slope, True), load_shares(number_of, rows * top, limit, slope, False)
    places = jnp.arange(number_of)

    def named(tallies, rotation):
        used = int((tallies > 0).sum())
        fixed = max(1, used // 4)
        moved = fixed + (places - fixed + rotation * (used - fixed)) % max(1, number_of - fixed)
        return jnp.zeros((number_of,), jnp.int32).at[sequence[jnp.where(places < fixed, places, moved)]].set(jnp.asarray(tallies, jnp.int32))

    tallies = jnp.where(number % 4 == 0, named(heavy_load, number // 4), named(common, number - number // 4 - 1))
    mixed = jax.random.permutation(jax.random.fold_in(own, 3), number_of)
    source_of, receiver = mixed[0:number_of // 2 * 2:2], mixed[1:number_of // 2 * 2:2]
    room = jnp.minimum(tallies[source_of] - 1, limit - tallies[receiver]) // 2
    room = jnp.where((source_of == sequence[0]) | (receiver == sequence[0]) | (tallies[receiver] == 0), 0, jnp.maximum(room, 0))
    moved = jax.random.randint(jax.random.fold_in(own, 4), (number_of // 2,), 0, 1 << 20) % (room + 1)
    tallies = tallies.at[source_of].add(-moved).at[receiver].add(moved)
    labels = jnp.searchsorted(jnp.cumsum(tallies), jnp.arange(rows * top), side="right").astype(jnp.int32)
    grid = labels.reshape(top, rows).T
    grid = grid[jax.random.permutation(jax.random.fold_in(own, 1), rows)]
    rotation = jax.random.randint(jax.random.fold_in(own, 2), (rows, 1), 0, top)
    return jnp.take_along_axis(grid, (jnp.arange(top)[None, :] + rotation) % top, axis=1)


def load_shares(count, total, reach, slope, full):
    weights = [(1 << 20) // math.isqrt(standing ** slope) + 1 for standing in range(1, count + 1)]
    largest = reach if full else min(reach, max(-(-total // count), total * weights[0] // sum(weights)))
    least = 1 if total - largest >= count - 1 else 0
    given, surplus = [largest] + [least] * (count - 1), total - largest - least * (count - 1)
    while surplus > 0:
        free = [i for i in range(1, count) if given[i] < largest] or [i for i in range(1, count) if given[i] < reach]
        mass, remaining = sum([weights[i] for i in free]), surplus
        for i in free:
            addition = min(reach - given[i], max(1, remaining * weights[i] // mass), surplus)
            given[i] = given[i] + addition
            surplus = surplus - addition
    return np.array(given)


def gaussian(own_key, shape, width, limit, shards=(), kind=jnp.bfloat16):
    factor_of = shard_levels(own_key, shape, shards, -0.22, 0.18) if shards else 1.0
    values = jax.random.normal(own_key, shape, jnp.float32) * width * factor_of
    return jnp.minimum(jnp.maximum(values, -limit), limit).astype(kind)


def setup_inputs(seed: int = 0) -> dict:
    key_list = jax.random.split(jax.random.key(seed), 14)
    hidden_in = gaussian(key_list[0], (TOKENS, D), 1.0, 6.0, ((0, 32),))
    query_latent = draw_query_latent(jax.random.fold_in(key_list[13], 71), 0)
    query_rope = draw_query_rope(jax.random.fold_in(key_list[13], 71), 0)
    cache_latent = draw_cache_latent(jax.random.fold_in(key_list[13], 71), 0)
    cache_rope = draw_cache_rope(jax.random.fold_in(key_list[13], 71), 0)
    lengths = plant(jax.random.randint(key_list[5], (TOKENS,), CTX // 8, CTX + 1), jax.random.fold_in(key_list[5], 1), CTX // 8, CTX).astype(jnp.int32)
    value_up = gaussian(key_list[6], (LAT, HEADS * HEAD_V), (LAT // 16) ** -0.5, 1.0, ((1, 4),))
    out_proj = gaussian(key_list[7], (HEADS * HEAD_V, D), (HEADS * HEAD_V) ** -0.5, 0.09375, ((0, 4),))
    norm_gain = jnp.clip(1.0 + 0.18 * jax.random.normal(key_list[8], (D,), jnp.float32), 0.1, 1.9)
    expert_gate = gaussian(key_list[9], (EXPERTS, D, FF), D ** -0.5, 0.09375, ((0, 32),))
    expert_down = gaussian(key_list[10], (EXPERTS, FF, D), FF ** -0.5, 0.1875, ((0, 32),))
    expert_ids_keys = jax.random.split(jax.random.fold_in(key_list[11], 1), TOKENS // TOK_DEV)
    expert_ids_turns = jax.random.permutation(jax.random.fold_in(key_list[11], 3), TOKENS // TOK_DEV)
    expert_ids = jax.vmap(lambda own, number: shared_out(jax.random.fold_in(key_list[11], 2), own, number, TOK_DEV, EXPERTS, TOPK, CAP, 2))(expert_ids_keys, expert_ids_turns).reshape((TOKENS, TOPK))
    affinity = jnp.clip(jnp.exp(math.log(1.0) - 2.9957323 * jax.random.uniform(key_list[12], (TOKENS, TOPK), jnp.float32) ** shard_levels(key_list[12], (TOKENS, TOPK), ((0, 32),), -0.2, 0.2)), 0.05, 1.0)
    return dict(hidden_in=hidden_in, query_latent=query_latent, query_rope=query_rope, cache_latent=cache_latent, cache_rope=cache_rope, lengths=lengths, value_up=value_up, out_proj=out_proj, norm_gain=norm_gain, expert_gate=expert_gate, expert_down=expert_down, expert_ids=expert_ids, affinity=affinity)


score_scale = 192.0 ** (-0.5)
norm_eps = 1e-06
route_scale = 2.5

def attend(query_latent, query_rope, cache_latent, cache_rope, lengths):
    token_count, head_count, latent_width = query_latent.shape
    rope_width = cache_rope.shape[1]
    context = cache_latent.shape[1]
    latent_wide = cache_latent.astype(jnp.float32)
    query_rot = query_rope.astype(jnp.float32).reshape(token_count, head_count, rope_width)
    scores = jnp.einsum('thl,tpl->thp', query_latent.astype(jnp.float32), latent_wide)
    scores = scores + jnp.einsum('thr,trp->thp', query_rot, cache_rope.astype(jnp.float32))
    scores = scores * score_scale
    position = lax.broadcasted_iota(jnp.int32, (token_count, 1, context), 2)
    scores = jnp.where(position < lengths.astype(jnp.int32)[:, None, None], scores, -jnp.inf)
    row_max = lax.optimization_barrier(jnp.max(scores, axis=2, keepdims=True))
    raised = jnp.exp(scores - row_max)
    attn_weights = (raised / lax.optimization_barrier(jnp.sum(raised, axis=2, keepdims=True))).astype(jnp.bfloat16)
    latent_out = jnp.einsum('thp,tpl->thl', attn_weights.astype(jnp.float32), latent_wide)
    return latent_out.astype(jnp.bfloat16)

def reference(hidden_in, query_latent, query_rope, cache_latent, cache_rope, lengths, value_up, out_proj, norm_gain, expert_gate, expert_down, expert_ids, affinity):
    latent_out = attend(query_latent, query_rope, cache_latent, cache_rope, lengths)
    up_table = value_up.astype(jnp.float32).reshape(LAT, HEADS, HEAD_V)
    per_head = jnp.einsum('thl,lhv->thv', latent_out.astype(jnp.float32), up_table).astype(jnp.bfloat16)
    attn_sum = jnp.dot(per_head.reshape(TOKENS, HEADS * HEAD_V), out_proj, preferred_element_type=jnp.float32)
    hidden = (hidden_in.astype(jnp.float32) + attn_sum).astype(jnp.bfloat16)
    wide_hidden = hidden.astype(jnp.float32)
    inv_norm = lax.rsqrt(lax.optimization_barrier(jnp.mean(wide_hidden * wide_hidden, axis=1, keepdims=True)) + norm_eps)
    normed = (wide_hidden * inv_norm * norm_gain.astype(jnp.float32)).astype(jnp.bfloat16)
    blocks = TOKENS // TOK_DEV
    per_block = TOK_DEV * TOPK
    block_ids = expert_ids.astype(jnp.int32).reshape(blocks, per_block)
    expert_iota = jnp.arange(EXPERTS, dtype=jnp.int32)
    one_hot = (block_ids[:, :, None] == expert_iota[None, None, :]).astype(jnp.int32)
    earlier = jnp.cumsum(one_hot, axis=1) - one_hot
    slot_index = lax.optimization_barrier(jnp.sum(earlier * one_hot, axis=2)).astype(jnp.int32)
    block_number = jnp.arange(blocks, dtype=jnp.int32)[:, None]
    target = (block_ids * (blocks * CAP) + block_number * CAP + slot_index).reshape(-1)
    owner_row = jnp.arange(TOKENS * TOPK, dtype=jnp.int32) // TOPK
    route_weight = route_scale * affinity / lax.optimization_barrier(jnp.sum(affinity, axis=1, keepdims=True))
    source_row = jnp.full((EXPERTS * blocks * CAP,), TOKENS, jnp.int32).at[target].set(owner_row)
    row_weight = jnp.zeros((EXPERTS * blocks * CAP,), jnp.float32).at[target].set(route_weight.reshape(-1))
    padded = jnp.concatenate([normed, jnp.zeros((1, D), jnp.bfloat16)], axis=0)

    def one_expert(total, inputs):
        rows_here, weights_here, gate_here, down_here = inputs
        inner_act = jax.nn.silu(jnp.dot(padded[rows_here], gate_here, preferred_element_type=jnp.float32)).astype(jnp.bfloat16)
        answer = jnp.dot(inner_act, down_here, preferred_element_type=jnp.float32).astype(jnp.bfloat16).astype(jnp.float32)
        return (total.at[rows_here].add(weights_here[:, None] * answer, mode='drop'), None)
    moe_sum = lax.scan(one_expert, jnp.zeros((TOKENS, D), jnp.float32), (source_row.reshape(EXPERTS, -1), row_weight.reshape(EXPERTS, -1), expert_gate, expert_down))[0]
    return (wide_hidden + moe_sum).astype(jnp.bfloat16)
```

```python
import functools
import types

import jax
import jax.numpy as jnp
from jax import lax
from jax.experimental import pallas as pl
from jax.experimental.pallas import tpu as pltpu
from jax.sharding import PartitionSpec as P

score_scale = 192.0 ** (-0.5)
norm_eps = 1e-06
route_scale = 2.5
low = jnp.bfloat16
wide = jnp.float32


def scratch_plan(size):
    tiles, tile, toks, outer, plane, per = size.tiles, size.tile, size.toks, size.outer, size.plane, size.per
    group, local, count = size.group, size.local, size.count
    dma = pltpu.SemaphoreType.DMA
    vmem = pltpu.VMEM
    lanes = size.lanes
    return dict(
        leaving=vmem((group, toks, local, size.latent), low),
        arrived=vmem((group, toks, local, size.latent), low),
        heads=vmem((group * toks, size.depth), low),
        partial=vmem((tiles, group, toks, tile), low),
        parts=vmem((tiles, group, toks, tile), low),
        total=vmem((tiles, toks, tile), wide),
        up=vmem((size.latent, size.depth), low),
        proj=vmem((size.depth, size.width), low),
        query=vmem((toks, size.heads, size.latent), low),
        cache=vmem((toks, size.context, size.latent), low),
        rope=vmem((toks, size.rope, size.context), low),
        rot=vmem((toks, size.heads * size.rope), low),
        turned=vmem((toks, size.heads, 128), low),
        hidden_in=vmem((toks, size.width), low),
        gain=vmem((size.width,), wide),
        meta=vmem((2 * size.topk, lanes), wide),
        meta_in=vmem((outer, 2 * size.topk, lanes), wide),
        pick=vmem((count, lanes), low),
        mix=vmem((2 * outer * toks, count), low),
        block=vmem((tiles, outer * toks, tile), low),
        sending=vmem((tiles, plane, per, tile), low),
        received=vmem((tiles, plane, per, tile), low),
        squares=vmem((count, 128), wide),
        acc=vmem((count, size.ff), wide),
        inner=vmem((count, size.ff), low),
        answers=vmem((tiles, plane, per, tile), low),
        back=vmem((tiles, plane, per, tile), low),
        owed=vmem((tiles, outer, toks, tile), low),
        owing=vmem((tiles, outer, toks, tile), low),
        gate=vmem((size.width, size.ff), low),
        down=vmem((size.ff, size.width), low),
        input_sem=dma((toks // size.batch, 3)),
        load_sem=dma((8,)),
        out_send=dma((toks // size.batch, group)),
        out_recv=dma((toks // size.batch, group)),
        part_send=dma((tiles, group)),
        part_recv=dma((tiles, group)),
        meta_send=dma((outer,)),
        meta_recv=dma((outer,)),
        far_send=dma((tiles, outer)),
        far_recv=dma((tiles, outer)),
        near_send=dma((tiles, plane)),
        near_recv=dma((tiles, plane)),
        back_send=dma((tiles, plane)),
        back_recv=dma((tiles, plane)),
        owed_send=dma((tiles, outer)),
        owed_recv=dma((tiles, outer)),
    )


def layer_kernel(
    size, names, query_hbm, rot_hbm, cache_hbm, rope_hbm, lengths_ref, hidden_hbm, gain_hbm, up_hbm, proj_hbm,
    meta_hbm, gate_hbm, down_hbm, out_ref, *refs,
):
    v = types.SimpleNamespace(**dict(zip(names, refs)))
    toks, batch, group, local, latent = size.toks, size.batch, size.group, size.local, size.latent
    tiles, tile, outer, plane, per, cap, count = (
        size.tiles, size.tile, size.outer, size.plane, size.per, size.cap, size.count
    )
    tp, inner_dp = size.tp, size.inner_dp
    head_count, context = size.heads, size.context
    at, my_tp = lax.axis_index("dp"), lax.axis_index("tp")
    level = lax.div(at, inner_dp)
    me = lax.rem(at, inner_dp) * tp + my_tp

    loads = {}

    def load(index, src, dst):
        loads[index] = pltpu.make_async_copy(src, dst, v.load_sem.at[index])
        loads[index].start()

    load(0, rot_hbm, v.rot)
    input_copies = []
    for number in range(toks // batch):
        span = pl.ds(number * batch, batch)
        pairs = ((query_hbm, v.query), (cache_hbm, v.cache), (rope_hbm, v.rope))
        input_copies.append([
            pltpu.make_async_copy(src.at[span], dst.at[span], v.input_sem.at[number, index])
            for index, (src, dst) in enumerate(pairs)
        ])
        for copy in input_copies[-1]:
            copy.start()
    load(1, meta_hbm, v.meta)
    load(2, up_hbm, v.up)
    load(3, proj_hbm, v.proj)
    load(4, hidden_hbm, v.hidden_in)
    load(5, gain_hbm, v.gain)

    def far(step):
        return {"dp": lax.rem(level + step, outer) * inner_dp + lax.rem(at, inner_dp), "tp": my_tp}

    def near(index):
        return {"dp": level * inner_dp + lax.div(index, tp), "tp": lax.rem(index, tp)}

    tp_peer = [lax.rem(my_tp + step, group) for step in range(group)]
    near_peer = [lax.rem(me + hop, plane) for hop in range(plane)]
    sent = []

    def remote(src, dst, send, recv, device):
        copy = pltpu.make_async_remote_copy(
            src_ref=src, dst_ref=dst, send_sem=send, recv_sem=recv,
            device_id=device, device_id_type=pl.DeviceIdType.MESH,
        )
        copy.start()
        sent.append(copy)
        return copy

    barrier = pltpu.get_barrier_semaphore()
    for step in range(1, outer):
        pl.semaphore_signal(barrier, inc=1, device_id=far(step), device_id_type=pl.DeviceIdType.MESH)
    for hop in range(1, plane):
        pl.semaphore_signal(barrier, inc=1, device_id=near(near_peer[hop]), device_id_type=pl.DeviceIdType.MESH)

    ratio = 128 // size.rope
    strips = head_count // ratio
    loads[0].wait()
    flat_rot = jnp.concatenate([v.rot[:, j * 128:(j + 1) * 128] for j in range(strips)], axis=0)
    spin_rows = batch * head_count
    spin_row = lax.broadcasted_iota(jnp.int32, (spin_rows, 1), 0)
    spin_lane = lax.broadcasted_iota(jnp.int32, (spin_rows, strips * toks), 1)
    head_of = lax.rem(spin_row, head_count)
    lane_of = lax.broadcasted_iota(jnp.int32, (spin_rows, 128), 1)
    own_lanes = lax.div(lane_of, size.rope) == lax.rem(head_of, ratio)
    for first in range(0, toks, batch):
        source = lax.div(head_of, ratio) * toks + lax.div(spin_row, head_count) + first
        spread = jnp.where(spin_lane == source, 1.0, 0.0).astype(low)
        moved = jnp.dot(spread, flat_rot, preferred_element_type=wide)
        moved = jnp.where(own_lanes, moved, 0.0).astype(low)
        v.turned[first:first + batch] = moved.reshape(batch, head_count, 128)

    position = lax.broadcasted_iota(jnp.int32, (head_count, context), 1)
    out_copies, meta_copies = {}, {}
    for first in range(0, toks, batch):
        for copy in input_copies[first // batch]:
            copy.wait()
        scores = []
        for t in range(first, first + batch):
            score = lax.dot_general(
                v.query[t], v.cache[t], (((1,), (1,)), ((), ())), preferred_element_type=wide
            )
            keys = jnp.concatenate([v.rope[t]] * ratio, axis=0)
            score = score + jnp.dot(v.turned[t], keys, preferred_element_type=wide)
            scores.append(jnp.where(position < lengths_ref[t], score * score_scale, -jnp.inf))
        weights = []
        for score in scores:
            raised = jnp.exp(score - jnp.max(score, axis=1, keepdims=True))
            weights.append((raised / jnp.sum(raised, axis=1, keepdims=True)).astype(low))
        for offset, weight in enumerate(weights):
            t = first + offset
            mixed = jnp.dot(weight, v.cache[t], preferred_element_type=wide).astype(low)
            for part in range(group):
                v.leaving[part, t] = mixed[part * local:(part + 1) * local]
        if first == 0:
            pl.semaphore_wait(barrier, outer + plane - 2)
        span = pl.ds(first, batch)
        number = first // batch
        for step in range(1, group):
            out_copies[number, step] = remote(
                v.leaving.at[tp_peer[step], span], v.arrived.at[step, span],
                v.out_send.at[number, step], v.out_recv.at[number, step], {"tp": tp_peer[step]},
            )
        if first == 0:
            loads[1].wait()
            for step in range(1, outer):
                meta_copies[step] = remote(
                    v.meta, v.meta_in.at[step], v.meta_send.at[step], v.meta_recv.at[step], far(step)
                )
            load(6, gate_hbm.at[0], v.gate)
            load(7, down_hbm.at[0], v.down)

    for step in range(1, outer):
        meta_copies[step].wait_recv()
    lanes, topk = size.lanes, size.topk
    step_of = lax.div(lax.broadcasted_iota(jnp.int32, (2 * topk, lanes), 1), toks)
    table = v.meta[...]
    for step in range(1, outer):
        table = jnp.where(step_of == step, v.meta_in[step], table)
    ids, affinity = table[:topk], table[topk:]
    shares = route_scale * affinity / jnp.sum(affinity, axis=0, keepdims=True)
    row = lax.broadcasted_iota(jnp.int32, (count, lanes), 0)
    lane = lax.broadcasted_iota(jnp.int32, (count, lanes), 1)
    expert = (level * plane + lax.div(row, per)).astype(wide)
    chosen = jnp.zeros((count, lanes), wide)
    share = jnp.zeros((count, lanes), wide)
    for k in range(topk):
        hit = ids[k:k + 1] == expert
        chosen = jnp.where(hit, 1.0, chosen)
        share = jnp.where(hit, shares[k:k + 1], share)
    older = lax.broadcasted_iota(jnp.int32, (lanes, lanes), 0)
    newer = lax.broadcasted_iota(jnp.int32, (lanes, lanes), 1)
    before = (older < newer) & (lax.div(older, toks) == lax.div(newer, toks))
    rank = jnp.dot(chosen.astype(low), jnp.where(before, 1.0, 0.0).astype(low), preferred_element_type=wide)
    slot = lax.rem(row, cap).astype(wide)
    own_step = lax.div(lane, toks) == lax.rem(lax.div(row, cap), outer)
    held = (chosen > 0.5) & own_step & (rank == slot)
    v.pick[...] = jnp.where(held, 1.0, 0.0).astype(low)
    flipped = jnp.where(held, share, 0.0).T
    high = flipped.astype(low)
    v.mix[:outer * toks] = high[:outer * toks]
    v.mix[outer * toks:] = (flipped - high.astype(wide)).astype(low)[:outer * toks]

    loads[2].wait()
    head_width = size.depth // local
    lane = lax.broadcasted_iota(jnp.int32, (local, size.depth), 1)
    row = lax.broadcasted_iota(jnp.int32, (local, size.depth), 0)
    own_head = lax.div(lane, head_width) == row
    for step in range(group):
        for first in range(0, toks, batch):
            if step:
                out_copies[first // batch, step].wait_recv()
        source = v.leaving[my_tp] if step == 0 else v.arrived[step]
        flat = source.reshape(toks * local, latent)
        for column in range(0, size.depth, 256):
            product = jnp.dot(flat, v.up[:, column:column + 256], preferred_element_type=wide)
            product = product.reshape(toks, local, 256)
            kept = jnp.where(own_head[None, :, column:column + 256], product, 0.0)
            v.heads[step * toks:(step + 1) * toks, column:column + 256] = jnp.sum(kept, axis=1).astype(low)
    loads[3].wait()
    part_copies = {}
    for n in range(tiles):
        product = jnp.dot(v.heads[...], v.proj[:, n * tile:(n + 1) * tile], preferred_element_type=wide)
        v.total[n] = product[:toks]
        for step in range(1, group):
            v.partial[n, step] = product[step * toks:(step + 1) * toks].astype(low)
            part_copies[n, step] = remote(
                v.partial.at[n, step], v.parts.at[n, step],
                v.part_send.at[n, step], v.part_recv.at[n, step], {"tp": tp_peer[group - step]},
            )
    loads[4].wait()
    far_copies = {}
    for n in range(tiles):
        value = v.total[n]
        for step in range(1, group):
            part_copies[n, step].wait_recv()
            value = value + v.parts[n, step].astype(wide)
        hidden = (v.hidden_in[:, n * tile:(n + 1) * tile].astype(wide) + value).astype(low)
        v.block[n, :toks] = hidden
        for step in range(1, outer):
            far_copies[n, step] = remote(
                v.block.at[n, pl.ds(0, toks)], v.block.at[n, pl.ds(step * toks, toks)],
                v.far_send.at[n, step], v.far_recv.at[n, step], far(step),
            )

    near_copies = {}

    def dispatch(n):
        for step in range(1, outer):
            far_copies[n, step].wait_recv()
        picked = jnp.dot(v.pick[:, :outer * toks], v.block[n], preferred_element_type=wide).astype(low)
        v.sending[n] = picked.reshape(plane, per, tile)
        for hop in range(1, plane):
            near_copies[n, hop] = remote(
                v.sending.at[n, near_peer[hop]], v.received.at[n, me],
                v.near_send.at[n, hop], v.near_recv.at[n, hop], near(near_peer[hop]),
            )
        v.received[n, me] = v.sending[n, me]

    def consume(n):
        for hop in range(1, plane):
            near_copies[n, hop].wait_recv()
        rows = v.received[n].reshape(count, tile).astype(wide)
        square = rows * rows
        folded = square[:, :128]
        for first in range(128, tile, 128):
            folded = folded + square[:, first:first + 128]
        gain = v.gain[pl.ds(n * tile, tile)]
        scaled = (rows * gain[None, :]).astype(low)
        product = jnp.dot(scaled, v.gate[n * tile:(n + 1) * tile, :], preferred_element_type=wide)
        if n == 0:
            v.squares[...] = folded
            v.acc[...] = product
        else:
            v.squares[...] += folded
            v.acc[...] += product

    loads[5].wait()
    lag = 3
    for n in range(tiles + lag):
        if n < tiles:
            dispatch(n)
        if n == lag:
            loads[6].wait()
        if n >= lag:
            consume(n - lag)
    inv_norm = lax.rsqrt(jnp.sum(v.squares[...], axis=1, keepdims=True) / size.width + norm_eps)
    v.inner[...] = jax.nn.silu(v.acc[...] * inv_norm).astype(low)
    loads[7].wait()

    back_copies, owed_copies = {}, {}
    for n in range(tiles):
        answer = jnp.dot(v.inner[...], v.down[:, n * tile:(n + 1) * tile], preferred_element_type=wide).astype(low)
        v.answers[n] = answer.reshape(plane, per, tile)
        for hop in range(1, plane):
            back_copies[n, hop] = remote(
                v.answers.at[n, near_peer[hop]], v.back.at[n, me],
                v.back_send.at[n, hop], v.back_recv.at[n, hop], near(near_peer[hop]),
            )
        v.back[n, me] = v.answers[n, me]

    def combine(n):
        for hop in range(1, plane):
            back_copies[n, hop].wait_recv()
        mixed = jnp.dot(v.mix[...], v.back[n].reshape(count, tile), preferred_element_type=wide)
        mixed = mixed[:outer * toks] + mixed[outer * toks:]
        v.total[n] = v.block[n, :toks].astype(wide) + mixed[:toks]
        for step in range(1, outer):
            v.owed[n, step] = mixed[step * toks:(step + 1) * toks].astype(low)
            owed_copies[n, step] = remote(
                v.owed.at[n, step], v.owing.at[n, step],
                v.owed_send.at[n, step], v.owed_recv.at[n, step], far(outer - step),
            )

    def finish(n):
        value = v.total[n]
        for step in range(1, outer):
            owed_copies[n, step].wait_recv()
            value = value + v.owing[n, step].astype(wide)
        out_ref[:, n * tile:(n + 1) * tile] = value.astype(low)

    for n in range(tiles + lag):
        if n < tiles:
            combine(n)
        if n >= lag:
            finish(n - lag)
    for copy in sent:
        copy.wait_send()


def per_device(
    hidden_in,
    query_latent,
    query_rope,
    cache_latent,
    cache_rope,
    lengths,
    value_up,
    out_proj,
    norm_gain,
    expert_gate,
    expert_down,
    expert_ids,
    affinity,
):
    toks, head_count, latent = query_latent.shape
    dp, tp = lax.axis_size("dp"), lax.axis_size("tp")
    inner_dp = 2 if dp % 2 == 0 else 1
    outer, plane = dp // inner_dp, inner_dp * tp
    experts = expert_gate.shape[0] * dp * tp
    cap = max(2, -(-expert_ids.size // experts))
    width, ff = expert_gate.shape[1:]
    tile = 512 if width % 512 == 0 else 128
    topk = expert_ids.shape[1]
    lanes = 128 * (-(-outer * toks // 128))
    size = types.SimpleNamespace(
        toks=toks, heads=head_count, latent=latent, context=cache_latent.shape[1], rope=cache_rope.shape[1],
        depth=out_proj.shape[0], width=width, ff=ff, group=tp, local=head_count // tp, tp=tp, inner_dp=inner_dp,
        outer=outer, plane=plane, cap=cap, per=outer * cap, count=plane * outer * cap, tile=tile,
        tiles=width // tile, batch=4 if toks % 4 == 0 else 1, topk=topk, lanes=lanes,
    )
    meta = jnp.concatenate([expert_ids.T.astype(wide), affinity.T], axis=0)
    meta = jnp.tile(meta, (1, lanes // toks))
    plan = scratch_plan(size)
    hbm = pl.BlockSpec(memory_space=pl.ANY)
    return pl.pallas_call(
        functools.partial(layer_kernel, size, tuple(plan)),
        out_shape=jax.ShapeDtypeStruct((toks, width), low),
        in_specs=[hbm] * 4 + [pl.BlockSpec(memory_space=pltpu.SMEM)] + [hbm] * 7,
        out_specs=pl.BlockSpec(memory_space=pltpu.VMEM),
        scratch_shapes=list(plan.values()),
        compiler_params=pltpu.CompilerParams(
            collective_id=0, has_side_effects=True, vmem_limit_bytes=60 * 1024 * 1024
        ),
    )(
        query_latent, query_rope, cache_latent, cache_rope, lengths, hidden_in, norm_gain, value_up, out_proj,
        meta, expert_gate, expert_down,
    )


def solution(mesh):
    spread = P(("dp", "tp"))
    return jax.shard_map(
        per_device,
        mesh=mesh,
        in_specs=(
            spread, spread, spread, spread, spread, spread, P(None, "tp"), P("tp", None), P(), spread, spread,
            spread, spread,
        ),
        out_specs=spread,
        check_vma=False,
    )
```

```python
import functools
import types

import jax
import jax.numpy as jnp
from jax import lax
from jax.experimental import pallas as pl
from jax.experimental.pallas import tpu as pltpu
from jax.sharding import PartitionSpec as P

score_scale = 192.0 ** (-0.5)
norm_eps = 1e-06
route_scale = 2.5
low = jnp.bfloat16
wide = jnp.float32


def scratch_plan(size):
    tiles, tile, toks, outer, plane, per = size.tiles, size.tile, size.toks, size.outer, size.plane, size.per
    group, local, count = size.group, size.local, size.count
    dma = pltpu.SemaphoreType.DMA
    vmem = pltpu.VMEM
    lanes = size.lanes
    return dict(
        leaving=vmem((group, toks, local, size.latent), low),
        arrived=vmem((group, toks, local, size.latent), low),
        heads=vmem((group * toks, size.depth), low),
        partial=vmem((tiles, 2, toks, tile), low),
        parts=vmem((tiles, 2, toks, tile), low),
        across=vmem((tiles, toks, tile), wide),
        crossing=vmem((tiles, toks, tile), low),
        crossed=vmem((tiles, toks, tile), low),
        total=vmem((tiles, toks, tile), wide),
        up=vmem((size.latent, size.depth), low),
        proj=vmem((size.depth, size.width), low),
        query=vmem((toks, size.heads, size.latent), low),
        cache=vmem((toks, size.context, size.latent), low),
        rope=vmem((toks, size.rope, size.context), low),
        rot=vmem((toks, size.heads * size.rope), low),
        hidden_in=vmem((toks, size.width), low),
        gain=vmem((size.width,), wide),
        ids=vmem((size.topk, toks), jnp.int32),
        affinity=vmem((size.topk, toks), wide),
        meta=vmem((2 * size.topk, lanes), wide),
        meta_in=vmem((outer, 2 * size.topk, lanes), wide),
        pick=vmem((count, lanes), low),
        mix=vmem((2 * outer * toks, count), low),
        block=vmem((tiles, outer * toks, tile), low),
        sending=vmem((tiles, plane, per, tile), low),
        received=vmem((tiles, plane, per, tile), low),
        squares=vmem((count, 128), wide),
        acc=vmem((count, size.ff), wide),
        inner=vmem((count, size.ff), low),
        answers=vmem((tiles, plane, per, tile), low),
        back=vmem((tiles, plane, per, tile), low),
        owed=vmem((tiles, outer, toks, tile), low),
        owing=vmem((tiles, outer, toks, tile), low),
        gate=vmem((size.width, size.ff), low),
        down=vmem((size.ff, size.width), low),
        lengths=pltpu.SMEM((toks,), jnp.int32),
        input_sem=dma((len(size.spans), 3)),
        load_sem=dma((10,)),
        send_sem=dma((8,)),
        out_recv=dma((size.halves, group)),
        pair_recv=dma((tiles,)),
        part_recv=dma((tiles,)),
        far_recv=dma((tiles,)),
        near_recv=dma((tiles,)),
        back_recv=dma((tiles,)),
        owed_recv=dma((tiles,)),
    )


def layer_kernel(
    size, names, query_hbm, rot_hbm, cache_hbm, rope_hbm, lengths_hbm, hidden_hbm, gain_hbm, up_hbm, proj_hbm,
    ids_hbm, affinity_hbm, gate_hbm, down_hbm, out_ref, *refs,
):
    v = types.SimpleNamespace(**dict(zip(names, refs)))
    toks, batch, group, local, latent = size.toks, size.batch, size.group, size.local, size.latent
    tiles, tile, outer, plane, per, cap, count = (
        size.tiles, size.tile, size.outer, size.plane, size.per, size.cap, size.count
    )
    tp, inner_dp = size.tp, size.inner_dp
    head_count, context = size.heads, size.context
    at, my_tp = lax.axis_index("dp"), lax.axis_index("tp")
    level = lax.div(at, inner_dp)
    me = lax.rem(at, inner_dp) * tp + my_tp

    def far(step):
        return {"dp": lax.rem(level + step, outer) * inner_dp + lax.rem(at, inner_dp), "tp": my_tp}

    def near(index):
        return {"dp": level * inner_dp + lax.div(index, tp), "tp": lax.rem(index, tp)}

    tp_peer = [my_tp, my_tp + 1 - 2 * lax.rem(my_tp, 2), lax.rem(my_tp + 2, 4), 3 - my_tp]
    near_peer = [lax.rem(me + hop, plane) for hop in range(plane)]

    def remote(src, dst, kind, recv, device):
        pltpu.make_async_remote_copy(
            src_ref=src, dst_ref=dst, send_sem=v.send_sem.at[kind], recv_sem=recv,
            device_id=device, device_id_type=pl.DeviceIdType.MESH,
        ).start()

    def settle(like, sem):
        pltpu.make_async_copy(like, like, sem).wait()

    barrier = pltpu.get_barrier_semaphore()
    for step in range(1, outer):
        pl.semaphore_signal(barrier, inc=1, device_id=far(step), device_id_type=pl.DeviceIdType.MESH)
    for hop in range(1, plane):
        pl.semaphore_signal(barrier, inc=1, device_id=near(near_peer[hop]), device_id_type=pl.DeviceIdType.MESH)

    loads = {}

    def load(index, src, dst):
        loads[index] = pltpu.make_async_copy(src, dst, v.load_sem.at[index])
        loads[index].start()

    load(0, rot_hbm, v.rot)
    load(9, lengths_hbm, v.lengths)
    input_copies = []
    for number, (first, extent) in enumerate(size.spans):
        span = pl.ds(first, extent)
        pairs = ((query_hbm, v.query), (cache_hbm, v.cache), (rope_hbm, v.rope))
        input_copies.append([
            pltpu.make_async_copy(src.at[span], dst.at[span], v.input_sem.at[number, index])
            for index, (src, dst) in enumerate(pairs)
        ])
        for copy in input_copies[-1]:
            copy.start()
    load(1, ids_hbm, v.ids)
    load(8, affinity_hbm, v.affinity)

    ratio = 128 // size.rope
    strips = head_count // ratio
    loads[0].wait()
    flat_rot = jnp.concatenate([v.rot[:, j * 128:(j + 1) * 128] for j in range(strips)], axis=0)
    spin_rows = batch * head_count
    spin_row = lax.broadcasted_iota(jnp.int32, (spin_rows, 1), 0)
    spin_lane = lax.broadcasted_iota(jnp.int32, (spin_rows, strips * toks), 1)
    head_of = lax.rem(spin_row, head_count)
    lane_of = lax.broadcasted_iota(jnp.int32, (spin_rows, 128), 1)
    own_lanes = lax.div(lane_of, size.rope) == lax.rem(head_of, ratio)

    def turned(first):
        source = lax.div(head_of, ratio) * toks + lax.div(spin_row, head_count) + first
        spread = jnp.where(spin_lane == source, 1.0, 0.0).astype(low)
        moved = jnp.dot(spread, flat_rot, preferred_element_type=wide)
        return jnp.where(own_lanes, moved, 0.0).astype(low).reshape(batch, head_count, 128)

    half = toks // size.halves
    position = lax.broadcasted_iota(jnp.int32, (head_count, context), 1)
    for first in range(0, toks, batch):
        spun = turned(first)
        for number, (begin, _) in enumerate(size.spans):
            if begin == first:
                for copy in input_copies[number]:
                    copy.wait()
        if first == 0:
            loads[9].wait()
            load(2, up_hbm, v.up)
            load(3, proj_hbm, v.proj)
            load(4, hidden_hbm, v.hidden_in)
            load(5, gain_hbm, v.gain)
        scores = []
        for t in range(first, first + batch):
            score = lax.dot_general(
                v.query[t], v.cache[t], (((1,), (1,)), ((), ())), preferred_element_type=wide
            )
            keys = jnp.concatenate([v.rope[t]] * ratio, axis=0)
            score = score + jnp.dot(spun[t - first], keys, preferred_element_type=wide)
            scores.append(jnp.where(position < v.lengths[t], score * score_scale, -jnp.inf))
        weights = []
        for score in scores:
            raised = jnp.exp(score - jnp.max(score, axis=1, keepdims=True))
            weights.append((raised / jnp.sum(raised, axis=1, keepdims=True)).astype(low))
        for offset, weight in enumerate(weights):
            t = first + offset
            mixed = jnp.dot(weight, v.cache[t], preferred_element_type=wide).astype(low)
            for part in range(group):
                v.leaving[part, t] = mixed[part * local:(part + 1) * local]
        if first == 0:
            pl.semaphore_wait(barrier, outer + plane - 2)
        span = pl.ds(first, batch)
        for step in range(group - 1, 0, -1):
            remote(
                v.leaving.at[tp_peer[step], span], v.arrived.at[step, span], 0,
                v.out_recv.at[first // half, step], {"tp": tp_peer[step]},
            )
        if first == 0:
            loads[1].wait()
            loads[8].wait()
            spot = lax.broadcasted_iota(jnp.int32, (toks, size.lanes), 0)
            copied = lax.rem(lax.broadcasted_iota(jnp.int32, (toks, size.lanes), 1), toks) == spot
            copied = jnp.where(copied, 1.0, 0.0)
            v.meta[:size.topk] = jnp.dot(
                v.ids[...].astype(wide), copied, precision=lax.Precision.HIGHEST, preferred_element_type=wide
            )
            v.meta[size.topk:] = jnp.dot(
                v.affinity[...], copied, precision=lax.Precision.HIGHEST, preferred_element_type=wide
            )
            for step in range(1, outer):
                remote(v.meta, v.meta_in.at[step], 1, v.out_recv.at[0, 0], far(step))
            load(6, gate_hbm.at[0], v.gate)
            load(7, down_hbm.at[0], v.down)

    settle(v.meta_in.at[pl.ds(1, outer - 1)], v.out_recv.at[0, 0])
    lanes, topk = size.lanes, size.topk
    step_of = lax.div(lax.broadcasted_iota(jnp.int32, (2 * topk, lanes), 1), toks)
    table = v.meta[...]
    for step in range(1, outer):
        table = jnp.where(step_of == step, v.meta_in[step], table)
    ids, affinity = table[:topk], table[topk:]
    shares = route_scale * affinity / jnp.sum(affinity, axis=0, keepdims=True)
    row = lax.broadcasted_iota(jnp.int32, (count, lanes), 0)
    lane = lax.broadcasted_iota(jnp.int32, (count, lanes), 1)
    expert = (level * plane + lax.div(row, per)).astype(wide)
    chosen = jnp.zeros((count, lanes), wide)
    share = jnp.zeros((count, lanes), wide)
    for k in range(topk):
        hit = ids[k:k + 1] == expert
        chosen = jnp.where(hit, 1.0, chosen)
        share = jnp.where(hit, shares[k:k + 1], share)
    older = lax.broadcasted_iota(jnp.int32, (lanes, lanes), 0)
    newer = lax.broadcasted_iota(jnp.int32, (lanes, lanes), 1)
    before = (older < newer) & (lax.div(older, toks) == lax.div(newer, toks))
    rank = jnp.dot(chosen.astype(low), jnp.where(before, 1.0, 0.0).astype(low), preferred_element_type=wide)
    slot = lax.rem(row, cap).astype(wide)
    own_step = lax.div(lane, toks) == lax.rem(lax.div(row, cap), outer)
    held = (chosen > 0.5) & own_step & (rank == slot)
    v.pick[...] = jnp.where(held, 1.0, 0.0).astype(low)
    flipped = jnp.where(held, share, 0.0).T
    high = flipped.astype(low)
    v.mix[:outer * toks] = high[:outer * toks]
    v.mix[outer * toks:] = (flipped - high.astype(wide)).astype(low)[:outer * toks]

    loads[2].wait()
    head_width = size.depth // local
    lane = lax.broadcasted_iota(jnp.int32, (local, size.depth), 1)
    row = lax.broadcasted_iota(jnp.int32, (local, size.depth), 0)
    own_head = lax.div(lane, head_width) == row
    for step in range(group):
        for begin in range(0, toks, half):
            span = pl.ds(begin, half)
            if step:
                settle(v.arrived.at[step, span], v.out_recv.at[begin // half, step])
            source = v.leaving[my_tp, span] if step == 0 else v.arrived[step, span]
            flat = source.reshape(half * local, latent)
            for column in range(0, size.depth, 256):
                product = jnp.dot(flat, v.up[:, column:column + 256], preferred_element_type=wide)
                product = product.reshape(half, local, 256)
                kept = jnp.where(own_head[None, :, column:column + 256], product, 0.0)
                value = jnp.sum(kept, axis=1).astype(low)
                v.heads[step * toks + begin:step * toks + begin + half, column:column + 256] = value
    loads[3].wait()

    def project(n):
        product = jnp.dot(v.heads[...], v.proj[:, n * tile:(n + 1) * tile], preferred_element_type=wide)
        v.total[n] = product[:toks]
        v.across[n] = product[2 * toks:3 * toks]
        v.partial[n, 0] = product[toks:2 * toks].astype(low)
        v.partial[n, 1] = product[3 * toks:].astype(low)
        remote(v.partial.at[n], v.parts.at[n], 2, v.pair_recv.at[n], {"tp": tp_peer[1]})

    def pass_on(n):
        settle(v.parts.at[n], v.pair_recv.at[n])
        v.total[n] += v.parts[n, 0].astype(wide)
        v.crossing[n] = (v.across[n] + v.parts[n, 1].astype(wide)).astype(low)
        remote(v.crossing.at[n], v.crossed.at[n], 3, v.part_recv.at[n], {"tp": tp_peer[2]})

    ahead = 3
    for n in range(tiles + ahead):
        if n < tiles:
            project(n)
        if n >= ahead:
            pass_on(n - ahead)
    loads[4].wait()
    for n in range(tiles):
        settle(v.crossed.at[n], v.part_recv.at[n])
        value = v.total[n] + v.crossed[n].astype(wide)
        hidden = (v.hidden_in[:, n * tile:(n + 1) * tile].astype(wide) + value).astype(low)
        v.block[n, :toks] = hidden
        for step in range(1, outer):
            remote(
                v.block.at[n, pl.ds(0, toks)], v.block.at[n, pl.ds(step * toks, toks)], 4, v.far_recv.at[n], far(step)
            )

    def dispatch(n):
        settle(v.block.at[n, pl.ds(toks, (outer - 1) * toks)], v.far_recv.at[n])
        picked = jnp.dot(v.pick[:, :outer * toks], v.block[n], preferred_element_type=wide).astype(low)
        v.sending[n] = picked.reshape(plane, per, tile)
        for hop in range(1, plane):
            remote(
                v.sending.at[n, near_peer[hop]], v.received.at[n, me], 5, v.near_recv.at[n], near(near_peer[hop])
            )
        v.received[n, me] = v.sending[n, me]

    def consume(n):
        settle(v.received.at[n, pl.ds(1, plane - 1)], v.near_recv.at[n])
        rows = v.received[n].reshape(count, tile).astype(wide)
        square = rows * rows
        folded = square[:, :128]
        for first in range(128, tile, 128):
            folded = folded + square[:, first:first + 128]
        gain = v.gain[pl.ds(n * tile, tile)]
        scaled = (rows * gain[None, :]).astype(low)
        product = jnp.dot(scaled, v.gate[n * tile:(n + 1) * tile, :], preferred_element_type=wide)
        if n == 0:
            v.squares[...] = folded
            v.acc[...] = product
        else:
            v.squares[...] += folded
            v.acc[...] += product

    loads[5].wait()
    lag = 3
    for n in range(tiles + lag):
        if n < tiles:
            dispatch(n)
        if n == lag:
            loads[6].wait()
        if n >= lag:
            consume(n - lag)
    inv_norm = lax.rsqrt(jnp.sum(v.squares[...], axis=1, keepdims=True) / size.width + norm_eps)
    v.inner[...] = jax.nn.silu(v.acc[...] * inv_norm).astype(low)
    loads[7].wait()

    for n in range(tiles):
        answer = jnp.dot(v.inner[...], v.down[:, n * tile:(n + 1) * tile], preferred_element_type=wide).astype(low)
        v.answers[n] = answer.reshape(plane, per, tile)
        for hop in range(1, plane):
            remote(v.answers.at[n, near_peer[hop]], v.back.at[n, me], 6, v.back_recv.at[n], near(near_peer[hop]))
        v.back[n, me] = v.answers[n, me]

    def combine(n):
        settle(v.back.at[n, pl.ds(1, plane - 1)], v.back_recv.at[n])
        mixed = jnp.dot(v.mix[...], v.back[n].reshape(count, tile), preferred_element_type=wide)
        mixed = mixed[:outer * toks] + mixed[outer * toks:]
        v.total[n] = v.block[n, :toks].astype(wide) + mixed[:toks]
        for step in range(1, outer):
            v.owed[n, step] = mixed[step * toks:(step + 1) * toks].astype(low)
            remote(v.owed.at[n, step], v.owing.at[n, step], 7, v.owed_recv.at[n], far(outer - step))

    def finish(n):
        value = v.total[n]
        settle(v.owing.at[n, pl.ds(1, outer - 1)], v.owed_recv.at[n])
        for step in range(1, outer):
            value = value + v.owing[n, step].astype(wide)
        out_ref[:, n * tile:(n + 1) * tile] = value.astype(low)

    for n in range(tiles + lag):
        if n < tiles:
            combine(n)
        if n >= lag:
            finish(n - lag)
    others = pl.ds(0, plane - 1)
    for kind, like in enumerate((
        v.leaving.at[pl.ds(0, group - 1)], v.meta_in.at[pl.ds(0, outer - 1)], v.partial, v.crossing,
        v.block.at[:, pl.ds(0, (outer - 1) * toks)], v.sending.at[:, others], v.answers.at[:, others],
        v.owed.at[:, pl.ds(0, outer - 1)],
    )):
        settle(like, v.send_sem.at[kind])


def per_device(
    hidden_in,
    query_latent,
    query_rope,
    cache_latent,
    cache_rope,
    lengths,
    value_up,
    out_proj,
    norm_gain,
    expert_gate,
    expert_down,
    expert_ids,
    affinity,
):
    toks, head_count, latent = query_latent.shape
    dp, tp = lax.axis_size("dp"), lax.axis_size("tp")
    inner_dp = 2 if dp % 2 == 0 else 1
    outer, plane = dp // inner_dp, inner_dp * tp
    experts = expert_gate.shape[0] * dp * tp
    cap = max(2, -(-expert_ids.size // experts))
    width, ff = expert_gate.shape[1:]
    tile = 512 if width % 512 == 0 else 128
    topk = expert_ids.shape[1]
    batch = 2 if toks % 2 == 0 else 1
    spans = [(0, batch), (batch, toks - batch)]
    if toks % 8 == 0:
        spans = [(0, batch), (batch, 4 - batch), (4, 4), (8, toks - 8)]
    lanes = 128 * (-(-outer * toks // 128))
    size = types.SimpleNamespace(
        toks=toks, heads=head_count, latent=latent, context=cache_latent.shape[1], rope=cache_rope.shape[1],
        depth=out_proj.shape[0], width=width, ff=ff, group=tp, local=head_count // tp, tp=tp, inner_dp=inner_dp,
        outer=outer, plane=plane, cap=cap, per=outer * cap, count=plane * outer * cap, tile=tile,
        tiles=width // tile, batch=batch, spans=spans, halves=2 if toks % 4 == 0 else 1, topk=topk, lanes=lanes,
    )
    plan = scratch_plan(size)
    hbm = pl.BlockSpec(memory_space=pl.ANY)
    return pl.pallas_call(
        functools.partial(layer_kernel, size, tuple(plan)),
        out_shape=jax.ShapeDtypeStruct((toks, width), low),
        in_specs=[hbm] * 13,
        out_specs=pl.BlockSpec(memory_space=pltpu.VMEM),
        scratch_shapes=list(plan.values()),
        compiler_params=pltpu.CompilerParams(
            collective_id=0, has_side_effects=True, vmem_limit_bytes=60 * 1024 * 1024
        ),
    )(
        query_latent, query_rope, cache_latent, cache_rope, lengths, hidden_in, norm_gain, value_up, out_proj,
        expert_ids.T, affinity.T, expert_gate, expert_down,
    )


def solution(mesh):
    spread = P(("dp", "tp"))
    return jax.shard_map(
        per_device,
        mesh=mesh,
        in_specs=(
            spread, spread, spread, spread, spread, spread, P(None, "tp"), P("tp", None), P(), spread, spread,
            spread, spread,
        ),
        out_specs=spread,
        check_vma=False,
    )
```

```python
import functools
import types

import jax
import jax.numpy as jnp
from jax import lax
from jax.experimental import pallas as pl
from jax.experimental.pallas import tpu as pltpu
from jax.sharding import PartitionSpec as P

score_scale = 192.0 ** (-0.5)
norm_eps = 1e-06
route_scale = 2.5
low = jnp.bfloat16
wide = jnp.float32


def scratch_plan(size):
    tiles, tile, toks, outer, plane, cap = size.tiles, size.tile, size.toks, size.outer, size.plane, size.cap
    group, local, count = size.group, size.local, size.count
    dma = pltpu.SemaphoreType.DMA
    vmem = pltpu.VMEM
    lanes = size.lanes
    return dict(
        leaving=vmem((group, toks, local, size.latent), low),
        arrived=vmem((group, toks, local, size.latent), low),
        heads=vmem((group * toks, size.depth), low),
        partial=vmem((tiles, 2, toks, tile), low),
        parts=vmem((tiles, 2, toks, tile), low),
        across=vmem((tiles, toks, tile), wide),
        crossing=vmem((tiles, toks, tile), low),
        crossed=vmem((tiles, toks, tile), low),
        total=vmem((tiles, toks, tile), wide),
        up=vmem((size.latent, size.depth), low),
        proj=vmem((size.depth, size.width), low),
        query=vmem((toks, size.heads, size.latent), low),
        cache=vmem((toks, size.context, size.latent), low),
        rope=vmem((toks, size.rope, size.context), low),
        rot=vmem((toks, size.heads * size.rope), low),
        hidden_in=vmem((toks, size.width), low),
        gain=vmem((size.width,), wide),
        ids=vmem((size.topk, toks), jnp.int32),
        affinity=vmem((size.topk, toks), wide),
        meta=vmem((2 * size.topk, lanes), wide),
        meta_in=vmem((outer, 2 * size.topk, lanes), wide),
        pick=vmem((count, lanes), low),
        mix=vmem((2 * outer * toks, count), low),
        block=vmem((tiles, outer * toks, tile), low),
        own_out=vmem((tiles, plane, cap, tile), low),
        own_in=vmem((tiles, plane, cap, tile), low),
        far_out=vmem((tiles, plane, outer - 1, cap, tile), low),
        far_in=vmem((tiles, plane, outer - 1, cap, tile), low),
        rows=vmem((2, count, tile), low),
        squares=vmem((count, 128), wide),
        acc=vmem((count, size.ff), wide),
        inner=vmem((count, size.ff), low),
        own_answers=vmem((tiles, plane, cap, tile), low),
        own_back=vmem((tiles, plane, cap, tile), low),
        far_answers=vmem((tiles, plane, outer - 1, cap, tile), low),
        far_back=vmem((tiles, plane, outer - 1, cap, tile), low),
        owed=vmem((tiles, outer, toks, tile), low),
        owing=vmem((tiles, outer, toks, tile), low),
        gate=vmem((size.width, size.ff), low),
        down=vmem((size.ff, size.width), low),
        lengths=pltpu.SMEM((toks,), jnp.int32),
        input_sem=dma((len(size.spans), 3)),
        load_sem=dma((10,)),
        send_sem=dma((10,)),
        out_recv=dma((size.halves, group)),
        pair_recv=dma((tiles,)),
        part_recv=dma((tiles,)),
        far_recv=dma((tiles, 2)),
        near_recv=dma((tiles, 2)),
        back_recv=dma((tiles, 2)),
        owed_recv=dma((tiles,)),
    )


def layer_kernel(
    size, names, query_hbm, rot_hbm, cache_hbm, rope_hbm, lengths_hbm, hidden_hbm, gain_hbm, up_hbm, proj_hbm,
    ids_hbm, affinity_hbm, gate_hbm, down_hbm, out_ref, *refs,
):
    v = types.SimpleNamespace(**dict(zip(names, refs)))
    toks, batch, group, local, latent = size.toks, size.batch, size.group, size.local, size.latent
    tiles, tile, outer, plane, cap, count = size.tiles, size.tile, size.outer, size.plane, size.cap, size.count
    tp, inner_dp = size.tp, size.inner_dp
    head_count, context = size.heads, size.context
    at, my_tp = lax.axis_index("dp"), lax.axis_index("tp")
    level = lax.div(at, inner_dp)
    me = lax.rem(at, inner_dp) * tp + my_tp

    def far(step):
        return {"dp": lax.rem(level + step, outer) * inner_dp + lax.rem(at, inner_dp), "tp": my_tp}

    def near(index):
        return {"dp": level * inner_dp + lax.div(index, tp), "tp": lax.rem(index, tp)}

    tp_peer = [my_tp, my_tp + 1 - 2 * lax.rem(my_tp, 2), lax.rem(my_tp + 2, 4), 3 - my_tp]
    near_peer = [lax.rem(me + hop, plane) for hop in range(plane)]

    def remote(src, dst, kind, recv, device):
        pltpu.make_async_remote_copy(
            src_ref=src, dst_ref=dst, send_sem=v.send_sem.at[kind], recv_sem=recv,
            device_id=device, device_id_type=pl.DeviceIdType.MESH,
        ).start()

    def settle(like, sem):
        pltpu.make_async_copy(like, like, sem).wait()

    barrier = pltpu.get_barrier_semaphore()
    for step in range(1, outer):
        pl.semaphore_signal(barrier, inc=1, device_id=far(step), device_id_type=pl.DeviceIdType.MESH)
    for hop in range(1, plane):
        pl.semaphore_signal(barrier, inc=1, device_id=near(near_peer[hop]), device_id_type=pl.DeviceIdType.MESH)

    loads = {}

    def load(index, src, dst):
        loads[index] = pltpu.make_async_copy(src, dst, v.load_sem.at[index])
        loads[index].start()

    load(0, rot_hbm, v.rot)
    load(9, lengths_hbm, v.lengths)
    input_copies = []
    for number, (first, extent) in enumerate(size.spans):
        span = pl.ds(first, extent)
        pairs = ((query_hbm, v.query), (cache_hbm, v.cache), (rope_hbm, v.rope))
        input_copies.append([
            pltpu.make_async_copy(src.at[span], dst.at[span], v.input_sem.at[number, index])
            for index, (src, dst) in enumerate(pairs)
        ])
        for copy in input_copies[-1]:
            copy.start()
    load(1, ids_hbm, v.ids)
    load(8, affinity_hbm, v.affinity)

    ratio = 128 // size.rope
    strips = head_count // ratio
    loads[0].wait()
    flat_rot = jnp.concatenate([v.rot[:, j * 128:(j + 1) * 128] for j in range(strips)], axis=0)
    spin_rows = batch * head_count
    spin_row = lax.broadcasted_iota(jnp.int32, (spin_rows, 1), 0)
    spin_lane = lax.broadcasted_iota(jnp.int32, (spin_rows, strips * toks), 1)
    head_of = lax.rem(spin_row, head_count)
    lane_of = lax.broadcasted_iota(jnp.int32, (spin_rows, 128), 1)
    own_lanes = lax.div(lane_of, size.rope) == lax.rem(head_of, ratio)

    def turned(first):
        source = lax.div(head_of, ratio) * toks + lax.div(spin_row, head_count) + first
        spread = jnp.where(spin_lane == source, 1.0, 0.0).astype(low)
        moved = jnp.dot(spread, flat_rot, preferred_element_type=wide)
        return jnp.where(own_lanes, moved, 0.0).astype(low).reshape(batch, head_count, 128)

    half = toks // size.halves
    position = lax.broadcasted_iota(jnp.int32, (head_count, context), 1)
    for first in range(0, toks, batch):
        spun = turned(first)
        for number, (begin, _) in enumerate(size.spans):
            if begin == first:
                for copy in input_copies[number]:
                    copy.wait()
        if first == 0:
            loads[9].wait()
            load(2, up_hbm, v.up)
            load(3, proj_hbm, v.proj)
            load(4, hidden_hbm, v.hidden_in)
            load(5, gain_hbm, v.gain)
        scores = []
        for t in range(first, first + batch):
            score = lax.dot_general(
                v.query[t], v.cache[t], (((1,), (1,)), ((), ())), preferred_element_type=wide
            )
            keys = jnp.concatenate([v.rope[t]] * ratio, axis=0)
            score = score + jnp.dot(spun[t - first], keys, preferred_element_type=wide)
            scores.append(jnp.where(position < v.lengths[t], score * score_scale, -jnp.inf))
        weights = []
        for score in scores:
            raised = jnp.exp(score - jnp.max(score, axis=1, keepdims=True))
            weights.append((raised / jnp.sum(raised, axis=1, keepdims=True)).astype(low))
        for offset, weight in enumerate(weights):
            t = first + offset
            mixed = jnp.dot(weight, v.cache[t], preferred_element_type=wide).astype(low)
            for part in range(group):
                v.leaving[part, t] = mixed[part * local:(part + 1) * local]
        if first == 0:
            pl.semaphore_wait(barrier, outer + plane - 2)
        span = pl.ds(first, batch)
        for step in range(group - 1, 0, -1):
            remote(
                v.leaving.at[tp_peer[step], span], v.arrived.at[step, span], 0,
                v.out_recv.at[first // half, step], {"tp": tp_peer[step]},
            )
        if first == 0:
            loads[1].wait()
            loads[8].wait()
            spot = lax.broadcasted_iota(jnp.int32, (toks, size.lanes), 0)
            copied = lax.rem(lax.broadcasted_iota(jnp.int32, (toks, size.lanes), 1), toks) == spot
            copied = jnp.where(copied, 1.0, 0.0)
            v.meta[:size.topk] = jnp.dot(
                v.ids[...].astype(wide), copied, precision=lax.Precision.HIGHEST, preferred_element_type=wide
            )
            v.meta[size.topk:] = jnp.dot(
                v.affinity[...], copied, precision=lax.Precision.HIGHEST, preferred_element_type=wide
            )
            for step in range(1, outer):
                remote(v.meta, v.meta_in.at[step], 1, v.out_recv.at[0, 0], far(step))
            load(6, gate_hbm.at[0], v.gate)
            load(7, down_hbm.at[0], v.down)

    settle(v.meta_in.at[pl.ds(1, outer - 1)], v.out_recv.at[0, 0])
    lanes, topk = size.lanes, size.topk
    step_of = lax.div(lax.broadcasted_iota(jnp.int32, (2 * topk, lanes), 1), toks)
    table = v.meta[...]
    for step in range(1, outer):
        table = jnp.where(step_of == step, v.meta_in[step], table)
    ids, affinity = table[:topk], table[topk:]
    shares = route_scale * affinity / jnp.sum(affinity, axis=0, keepdims=True)
    row = lax.broadcasted_iota(jnp.int32, (count, lanes), 0)
    lane = lax.broadcasted_iota(jnp.int32, (count, lanes), 1)
    mine = plane * cap
    rest = row - mine
    near_index = jnp.where(row < mine, lax.div(row, cap), lax.div(rest, (outer - 1) * cap))
    row_step = jnp.where(row < mine, 0, 1 + lax.rem(lax.div(rest, cap), outer - 1))
    expert = (level * plane + near_index).astype(wide)
    chosen = jnp.zeros((count, lanes), wide)
    share = jnp.zeros((count, lanes), wide)
    for k in range(topk):
        hit = ids[k:k + 1] == expert
        chosen = jnp.where(hit, 1.0, chosen)
        share = jnp.where(hit, shares[k:k + 1], share)
    older = lax.broadcasted_iota(jnp.int32, (lanes, lanes), 0)
    newer = lax.broadcasted_iota(jnp.int32, (lanes, lanes), 1)
    before = (older < newer) & (lax.div(older, toks) == lax.div(newer, toks))
    rank = jnp.dot(chosen.astype(low), jnp.where(before, 1.0, 0.0).astype(low), preferred_element_type=wide)
    slot = lax.rem(row, cap).astype(wide)
    own_step = lax.div(lane, toks) == row_step
    held = (chosen > 0.5) & own_step & (rank == slot)
    v.pick[...] = jnp.where(held, 1.0, 0.0).astype(low)
    flipped = jnp.where(held, share, 0.0).T
    high = flipped.astype(low)
    v.mix[:outer * toks] = high[:outer * toks]
    v.mix[outer * toks:] = (flipped - high.astype(wide)).astype(low)[:outer * toks]

    loads[2].wait()
    head_width = size.depth // local
    lane = lax.broadcasted_iota(jnp.int32, (local, size.depth), 1)
    row = lax.broadcasted_iota(jnp.int32, (local, size.depth), 0)
    own_head = lax.div(lane, head_width) == row
    for step in range(group):
        for begin in range(0, toks, half):
            span = pl.ds(begin, half)
            if step:
                settle(v.arrived.at[step, span], v.out_recv.at[begin // half, step])
            source = v.leaving[my_tp, span] if step == 0 else v.arrived[step, span]
            flat = source.reshape(half * local, latent)
            for column in range(0, size.depth, 256):
                product = jnp.dot(flat, v.up[:, column:column + 256], preferred_element_type=wide)
                product = product.reshape(half, local, 256)
                kept = jnp.where(own_head[None, :, column:column + 256], product, 0.0)
                value = jnp.sum(kept, axis=1).astype(low)
                v.heads[step * toks + begin:step * toks + begin + half, column:column + 256] = value
    loads[3].wait()

    def project(n):
        product = jnp.dot(v.heads[...], v.proj[:, n * tile:(n + 1) * tile], preferred_element_type=wide)
        v.total[n] = product[:toks]
        v.across[n] = product[2 * toks:3 * toks]
        v.partial[n, 0] = product[toks:2 * toks].astype(low)
        v.partial[n, 1] = product[3 * toks:].astype(low)
        remote(v.partial.at[n], v.parts.at[n], 2, v.pair_recv.at[n], {"tp": tp_peer[1]})

    def pass_on(n):
        settle(v.parts.at[n], v.pair_recv.at[n])
        v.total[n] += v.parts[n, 0].astype(wide)
        v.crossing[n] = (v.across[n] + v.parts[n, 1].astype(wide)).astype(low)
        remote(v.crossing.at[n], v.crossed.at[n], 3, v.part_recv.at[n], {"tp": tp_peer[2]})

    ahead = 3
    for n in range(tiles + ahead):
        if n < tiles:
            project(n)
        if n >= ahead:
            pass_on(n - ahead)
    line = outer == 4
    edge = (level == 0) | (level == outer - 1)

    def to_level(n, step):
        remote(v.block.at[n, pl.ds(0, toks)], v.block.at[n, pl.ds(step * toks, toks)], 4, v.far_recv.at[n, step % 2], far(step))

    def near_sends(out, into, kind, recv):
        for hop in range(1, plane):
            remote(out.at[near_peer[hop]], into.at[me], kind, recv, near(near_peer[hop]))

    def residual(n):
        settle(v.crossed.at[n], v.part_recv.at[n])
        value = v.total[n] + v.crossed[n].astype(wide)
        hidden = (v.hidden_in[:, n * tile:(n + 1) * tile].astype(wide) + value).astype(low)
        v.block[n, :toks] = hidden
        for step in range(1, outer):
            if line and step == 1:
                pl.when(level != outer - 1)(functools.partial(to_level, n, step))
            elif line and step == outer - 1:
                pl.when(level != 0)(functools.partial(to_level, n, step))
            else:
                to_level(n, step)
        picked = jnp.dot(v.pick[:mine, :toks], hidden, preferred_element_type=wide).astype(low)
        for index in range(plane):
            v.own_out[n, index] = picked[index * cap:(index + 1) * cap]
        near_sends(v.own_out.at[n], v.own_in.at[n], 5, v.near_recv.at[n, 0])
        v.own_in[n, me] = v.own_out[n, me]

    def relay(n):
        settle(v.block.at[n, pl.ds(0, (outer // 2 - (0 if outer % 2 else 1)) * toks)], v.far_recv.at[n, 0])
        if line:
            def pass_up():
                remote(
                    v.block.at[n, pl.ds(2 * toks, toks)], v.block.at[n, pl.ds(3 * toks, toks)], 4,
                    v.far_recv.at[n, 1], far(1),
                )

            def pass_down():
                remote(
                    v.block.at[n, pl.ds(2 * toks, toks)], v.block.at[n, pl.ds(toks, toks)], 4,
                    v.far_recv.at[n, 1], far(3),
                )

            pl.when(level == 2)(pass_up)
            pl.when(level == 1)(pass_down)

    def dispatch(n):
        settle(v.block.at[n, pl.ds(0, outer // 2 * toks)], v.far_recv.at[n, 1])
        picked = jnp.dot(
            v.pick[mine:, :outer * toks], v.block[n], preferred_element_type=wide
        ).astype(low)
        for index in range(plane):
            for step in range(outer - 1):
                first = (index * (outer - 1) + step) * cap
                v.far_out[n, index, step] = picked[first:first + cap]
        near_sends(v.far_out.at[n], v.far_in.at[n], 6, v.near_recv.at[n, 1])
        v.far_in[n, me] = v.far_out[n, me]

    def gather(own, distant, into):
        for index in range(plane):
            into[index * cap:(index + 1) * cap] = own[index]
            for step in range(outer - 1):
                first = mine + (index * (outer - 1) + step) * cap
                into[first:first + cap] = distant[index, step]

    def consume(n):
        settle(v.own_in.at[n, pl.ds(0, plane - 1)], v.near_recv.at[n, 0])
        settle(v.far_in.at[n, pl.ds(0, plane - 1)], v.near_recv.at[n, 1])
        into = v.rows.at[n % 2]
        gather(v.own_in.at[n], v.far_in.at[n], into)
        rows = into[...].astype(wide)
        square = rows * rows
        folded = square[:, :128]
        for first in range(128, tile, 128):
            folded = folded + square[:, first:first + 128]
        gain = v.gain[pl.ds(n * tile, tile)]
        scaled = (rows * gain[None, :]).astype(low)
        product = jnp.dot(scaled, v.gate[n * tile:(n + 1) * tile, :], preferred_element_type=wide)
        if n == 0:
            v.squares[...] = folded
            v.acc[...] = product
        else:
            v.squares[...] += folded
            v.acc[...] += product

    loads[4].wait()
    for n in range(tiles):
        residual(n)
    loads[5].wait()
    loads[6].wait()
    behind, lag = 1, 4
    for n in range(tiles + lag):
        if n < tiles:
            relay(n)
        if behind <= n < tiles + behind:
            dispatch(n - behind)
        if n >= lag:
            consume(n - lag)
    inv_norm = lax.rsqrt(jnp.sum(v.squares[...], axis=1, keepdims=True) / size.width + norm_eps)
    v.inner[...] = jax.nn.silu(v.acc[...] * inv_norm).astype(low)
    loads[7].wait()

    for n in range(tiles):
        answer = jnp.dot(v.inner[...], v.down[:, n * tile:(n + 1) * tile], preferred_element_type=wide).astype(low)
        for index in range(plane):
            v.own_answers[n, index] = answer[index * cap:(index + 1) * cap]
            for step in range(outer - 1):
                first = mine + (index * (outer - 1) + step) * cap
                v.far_answers[n, index, step] = answer[first:first + cap]
        near_sends(v.far_answers.at[n], v.far_back.at[n], 7, v.back_recv.at[n, 1])
        v.far_back[n, me] = v.far_answers[n, me]
    for n in range(tiles):
        near_sends(v.own_answers.at[n], v.own_back.at[n], 8, v.back_recv.at[n, 0])
        v.own_back[n, me] = v.own_answers[n, me]

    def combine(n):
        settle(v.far_back.at[n, pl.ds(0, plane - 1)], v.back_recv.at[n, 1])
        into = v.rows.at[n % 2]
        for index in range(plane):
            for step in range(outer - 1):
                first = mine + (index * (outer - 1) + step) * cap
                into[first:first + cap] = v.far_back[n, index, step]
        mixed = jnp.dot(v.mix[:, mine:], into[mine:], preferred_element_type=wide)
        mixed = mixed[:outer * toks] + mixed[outer * toks:]
        for step in range(1, outer):
            v.owed[n, step] = mixed[step * toks:(step + 1) * toks].astype(low)
            remote(v.owed.at[n, step], v.owing.at[n, step], 9, v.owed_recv.at[n], far(outer - step))

    def finish(n):
        settle(v.own_back.at[n, pl.ds(0, plane - 1)], v.back_recv.at[n, 0])
        into = v.rows.at[n % 2]
        for index in range(plane):
            into[index * cap:(index + 1) * cap] = v.own_back[n, index]
        mixed = jnp.dot(v.mix[:, :mine], into[:mine], preferred_element_type=wide)
        value = v.block[n, :toks].astype(wide) + mixed[:toks] + mixed[outer * toks:outer * toks + toks]
        settle(v.owing.at[n, pl.ds(1, outer - 1)], v.owed_recv.at[n])
        for step in range(1, outer):
            value = value + v.owing[n, step].astype(wide)
        out_ref[:, n * tile:(n + 1) * tile] = value.astype(low)

    for n in range(tiles):
        combine(n)
    for n in range(tiles):
        finish(n)
    others = pl.ds(0, plane - 1)
    for kind, like in enumerate((
        v.leaving.at[pl.ds(0, group - 1)], v.meta_in.at[pl.ds(0, outer - 1)], v.partial, v.crossing,
        None, v.own_out.at[:, others], v.far_out.at[:, others], v.far_answers.at[:, others],
        v.own_answers.at[:, others], v.owed.at[:, pl.ds(0, outer - 1)],
    )):
        if like is not None:
            settle(like, v.send_sem.at[kind])
    if line:
        pl.when(edge)(lambda: settle(v.block.at[:, pl.ds(0, 2 * toks)], v.send_sem.at[4]))
        pl.when(jnp.logical_not(edge))(lambda: settle(v.block, v.send_sem.at[4]))
    else:
        settle(v.block.at[:, pl.ds(0, (outer - 1) * toks)], v.send_sem.at[4])


def per_device(
    hidden_in,
    query_latent,
    query_rope,
    cache_latent,
    cache_rope,
    lengths,
    value_up,
    out_proj,
    norm_gain,
    expert_gate,
    expert_down,
    expert_ids,
    affinity,
):
    toks, head_count, latent = query_latent.shape
    dp, tp = lax.axis_size("dp"), lax.axis_size("tp")
    inner_dp = 2 if dp % 2 == 0 else 1
    outer, plane = dp // inner_dp, inner_dp * tp
    experts = expert_gate.shape[0] * dp * tp
    cap = max(2, -(-expert_ids.size // experts))
    width, ff = expert_gate.shape[1:]
    tile = 512 if width % 512 == 0 else 128
    topk = expert_ids.shape[1]
    batch = 2 if toks % 2 == 0 else 1
    spans = [(0, batch), (batch, toks - batch)]
    if toks % 8 == 0:
        spans = [(0, batch), (batch, 4 - batch), (4, 4), (8, toks - 8)]
    lanes = 128 * (-(-outer * toks // 128))
    size = types.SimpleNamespace(
        toks=toks, heads=head_count, latent=latent, context=cache_latent.shape[1], rope=cache_rope.shape[1],
        depth=out_proj.shape[0], width=width, ff=ff, group=tp, local=head_count // tp, tp=tp, inner_dp=inner_dp,
        outer=outer, plane=plane, cap=cap, count=plane * outer * cap, tile=tile,
        tiles=width // tile, batch=batch, spans=spans, halves=2 if toks % 4 == 0 else 1, topk=topk, lanes=lanes,
    )
    plan = scratch_plan(size)
    hbm = pl.BlockSpec(memory_space=pl.ANY)
    return pl.pallas_call(
        functools.partial(layer_kernel, size, tuple(plan)),
        out_shape=pltpu.VMEM((toks, width), low),
        in_specs=[hbm] * 13,
        out_specs=pl.BlockSpec(memory_space=pltpu.VMEM),
        scratch_shapes=list(plan.values()),
        compiler_params=pltpu.CompilerParams(
            collective_id=0, has_side_effects=True, vmem_limit_bytes=60 * 1024 * 1024
        ),
    )(
        query_latent, query_rope, cache_latent, cache_rope, lengths, hidden_in, norm_gain, value_up, out_proj,
        expert_ids.T, affinity.T, expert_gate, expert_down,
    )


def solution(mesh):
    spread = P(("dp", "tp"))
    return jax.shard_map(
        per_device,
        mesh=mesh,
        in_specs=(
            spread, spread, spread, spread, spread, spread, P(None, "tp"), P("tp", None), P(), spread, spread,
            spread, spread,
        ),
        out_specs=spread,
        check_vma=False,
    )
```

```python
import functools
import types

import jax
import jax.numpy as jnp
from jax import lax
from jax.experimental import pallas as pl
from jax.experimental.pallas import tpu as pltpu
from jax.sharding import PartitionSpec as P

score_scale = 192.0 ** (-0.5)
norm_eps = 1e-06
route_scale = 2.5
low = jnp.bfloat16
wide = jnp.float32


def scratch_plan(size):
    tiles, tile, toks, outer, plane, cap = size.tiles, size.tile, size.toks, size.outer, size.plane, size.cap
    group, local, count = size.group, size.local, size.count
    dma = pltpu.SemaphoreType.DMA
    vmem = pltpu.VMEM
    lanes = size.lanes
    return dict(
        leaving=vmem((group, toks, local, size.latent), low),
        arrived=vmem((group, toks, local, size.latent), low),
        heads=vmem((group * toks, size.depth), low),
        partial=vmem((tiles, 2, toks, tile), low),
        parts=vmem((tiles, 2, toks, tile), low),
        across=vmem((tiles, toks, tile), wide),
        crossing=vmem((tiles, toks, tile), low),
        crossed=vmem((tiles, toks, tile), low),
        total=vmem((tiles, toks, tile), wide),
        up=vmem((size.latent, size.depth), low),
        proj=vmem((size.depth, size.width), low),
        query=vmem((toks, size.heads, size.latent), low),
        cache=vmem((toks, size.context, size.latent), low),
        rope=vmem((toks, size.rope, size.context), low),
        rot=vmem((toks, size.heads * size.rope), low),
        hidden_in=vmem((toks, size.width), low),
        gain=vmem((size.width,), wide),
        ids=vmem((size.topk, toks), jnp.int32),
        affinity=vmem((size.topk, toks), wide),
        meta=vmem((2 * size.topk, lanes), wide),
        meta_in=vmem((outer, 2 * size.topk, lanes), wide),
        pick=vmem((count, lanes), low),
        mix=vmem((2 * outer * toks, count), low),
        block=vmem((tiles, outer * toks, tile), low),
        own_out=vmem((tiles, plane, cap, tile), low),
        own_in=vmem((tiles, plane, cap, tile), low),
        far_out=vmem((tiles, plane, outer - 1, cap, tile), low),
        far_in=vmem((tiles, plane, outer - 1, cap, tile), low),
        rows=vmem((2, count, tile), low),
        squares=vmem((count, 128), wide),
        acc=vmem((count, size.ff), wide),
        inner=vmem((count, size.ff), low),
        own_answers=vmem((tiles, plane, cap, tile), low),
        own_back=vmem((tiles, plane, cap, tile), low),
        far_answers=vmem((tiles, plane, outer - 1, cap, tile), low),
        far_back=vmem((tiles, plane, outer - 1, cap, tile), low),
        owed=vmem((tiles, outer, toks, tile), low),
        owing=vmem((tiles, outer, toks, tile), low),
        gate=vmem((size.width, size.ff), low),
        down=vmem((size.ff, size.width), low),
        lengths=pltpu.SMEM((toks,), jnp.int32),
        input_sem=dma((len(size.spans), 3)),
        load_sem=dma((10,)),
        send_sem=dma((10,)),
        out_recv=dma((size.halves, group)),
        pair_recv=dma((tiles,)),
        part_recv=dma((tiles,)),
        far_recv=dma((tiles, 2)),
        near_recv=dma((tiles, 2)),
        back_recv=dma((tiles, 2)),
        owed_recv=dma((tiles,)),
    )


def layer_kernel(
    size, names, query_hbm, rot_hbm, cache_hbm, rope_hbm, lengths_hbm, hidden_hbm, gain_hbm, up_hbm, proj_hbm,
    ids_hbm, affinity_hbm, gate_hbm, down_hbm, out_ref, *refs,
):
    v = types.SimpleNamespace(**dict(zip(names, refs)))
    toks, batch, group, local, latent = size.toks, size.batch, size.group, size.local, size.latent
    tiles, tile, outer, plane, cap, count = size.tiles, size.tile, size.outer, size.plane, size.cap, size.count
    tp, inner_dp = size.tp, size.inner_dp
    head_count, context = size.heads, size.context
    at, my_tp = lax.axis_index("dp"), lax.axis_index("tp")
    level = lax.div(at, inner_dp)
    me = lax.rem(at, inner_dp) * tp + my_tp

    def far(step):
        return {"dp": lax.rem(level + step, outer) * inner_dp + lax.rem(at, inner_dp), "tp": my_tp}

    def near(index):
        return {"dp": level * inner_dp + lax.div(index, tp), "tp": lax.rem(index, tp)}

    tp_peer = [my_tp, my_tp + 1 - 2 * lax.rem(my_tp, 2), lax.rem(my_tp + 2, 4), 3 - my_tp]
    near_peer = [lax.rem(me + hop, plane) for hop in range(plane)]

    def remote(src, dst, kind, recv, device):
        pltpu.make_async_remote_copy(
            src_ref=src, dst_ref=dst, send_sem=v.send_sem.at[kind], recv_sem=recv,
            device_id=device, device_id_type=pl.DeviceIdType.MESH,
        ).start()

    def settle(like, sem):
        pltpu.make_async_copy(like, like, sem).wait()

    barrier = pltpu.get_barrier_semaphore()
    for step in range(1, outer):
        pl.semaphore_signal(barrier, inc=1, device_id=far(step), device_id_type=pl.DeviceIdType.MESH)
    for hop in range(1, plane):
        pl.semaphore_signal(barrier, inc=1, device_id=near(near_peer[hop]), device_id_type=pl.DeviceIdType.MESH)

    loads = {}

    def load(index, src, dst):
        loads[index] = pltpu.make_async_copy(src, dst, v.load_sem.at[index])
        loads[index].start()

    load(0, rot_hbm, v.rot)
    load(9, lengths_hbm, v.lengths)
    input_copies = []
    for number, (first, extent) in enumerate(size.spans):
        span = pl.ds(first, extent)
        pairs = ((query_hbm, v.query), (cache_hbm, v.cache), (rope_hbm, v.rope))
        input_copies.append([
            pltpu.make_async_copy(src.at[span], dst.at[span], v.input_sem.at[number, index])
            for index, (src, dst) in enumerate(pairs)
        ])
        for copy in input_copies[-1]:
            copy.start()
    load(1, ids_hbm, v.ids)
    load(8, affinity_hbm, v.affinity)

    ratio = 128 // size.rope
    strips = head_count // ratio
    loads[0].wait()
    flat_rot = jnp.concatenate([v.rot[:, j * 128:(j + 1) * 128] for j in range(strips)], axis=0)
    spin_rows = batch * head_count
    spin_row = lax.broadcasted_iota(jnp.int32, (spin_rows, 1), 0)
    spin_lane = lax.broadcasted_iota(jnp.int32, (spin_rows, strips * toks), 1)
    head_of = lax.rem(spin_row, head_count)
    lane_of = lax.broadcasted_iota(jnp.int32, (spin_rows, 128), 1)
    own_lanes = lax.div(lane_of, size.rope) == lax.rem(head_of, ratio)

    def turned(first):
        source = lax.div(head_of, ratio) * toks + lax.div(spin_row, head_count) + first
        spread = jnp.where(spin_lane == source, 1.0, 0.0).astype(low)
        moved = jnp.dot(spread, flat_rot, preferred_element_type=wide)
        return jnp.where(own_lanes, moved, 0.0).astype(low).reshape(batch, head_count, 128)

    half = toks // size.halves
    position = lax.broadcasted_iota(jnp.int32, (head_count, context), 1)
    for first in range(0, toks, batch):
        spun = turned(first)
        for number, (begin, _) in enumerate(size.spans):
            if begin == first:
                for copy in input_copies[number]:
                    copy.wait()
        if first == 0:
            loads[9].wait()
            load(2, up_hbm, v.up)
            load(3, proj_hbm, v.proj)
            load(4, hidden_hbm, v.hidden_in)
            load(5, gain_hbm, v.gain)
        scores = []
        for t in range(first, first + batch):
            score = lax.dot_general(
                v.query[t], v.cache[t], (((1,), (1,)), ((), ())), preferred_element_type=wide
            )
            keys = jnp.concatenate([v.rope[t]] * ratio, axis=0)
            score = score + jnp.dot(spun[t - first], keys, preferred_element_type=wide)
            scores.append(jnp.where(position < v.lengths[t], score * score_scale, -jnp.inf))
        weights = []
        for score in scores:
            raised = jnp.exp(score - jnp.max(score, axis=1, keepdims=True))
            weights.append((raised / jnp.sum(raised, axis=1, keepdims=True)).astype(low))
        for offset, weight in enumerate(weights):
            t = first + offset
            mixed = jnp.dot(weight, v.cache[t], preferred_element_type=wide).astype(low)
            for part in range(group):
                v.leaving[part, t] = mixed[part * local:(part + 1) * local]
        if first == 0:
            pl.semaphore_wait(barrier, outer + plane - 2)
        span = pl.ds(first, batch)
        for step in range(group - 1, 0, -1):
            remote(
                v.leaving.at[tp_peer[step], span], v.arrived.at[step, span], 0,
                v.out_recv.at[first // half, step], {"tp": tp_peer[step]},
            )
        if first == 0:
            loads[1].wait()
            loads[8].wait()
            spot = lax.broadcasted_iota(jnp.int32, (toks, size.lanes), 0)
            copied = lax.rem(lax.broadcasted_iota(jnp.int32, (toks, size.lanes), 1), toks) == spot
            copied = jnp.where(copied, 1.0, 0.0)
            v.meta[:size.topk] = jnp.dot(
                v.ids[...].astype(wide), copied, precision=lax.Precision.HIGHEST, preferred_element_type=wide
            )
            v.meta[size.topk:] = jnp.dot(
                v.affinity[...], copied, precision=lax.Precision.HIGHEST, preferred_element_type=wide
            )
            for step in range(1, outer):
                remote(v.meta, v.meta_in.at[step], 1, v.out_recv.at[0, 0], far(step))
            load(6, gate_hbm.at[0], v.gate)
            load(7, down_hbm.at[0], v.down)

    settle(v.meta_in.at[pl.ds(1, outer - 1)], v.out_recv.at[0, 0])
    lanes, topk = size.lanes, size.topk
    step_of = lax.div(lax.broadcasted_iota(jnp.int32, (2 * topk, lanes), 1), toks)
    table = v.meta[...]
    for step in range(1, outer):
        table = jnp.where(step_of == step, v.meta_in[step], table)
    ids, affinity = table[:topk], table[topk:]
    shares = route_scale * affinity / jnp.sum(affinity, axis=0, keepdims=True)
    row = lax.broadcasted_iota(jnp.int32, (count, lanes), 0)
    lane = lax.broadcasted_iota(jnp.int32, (count, lanes), 1)
    mine = plane * cap
    rest = row - mine
    near_index = jnp.where(row < mine, lax.div(row, cap), lax.div(rest, (outer - 1) * cap))
    row_step = jnp.where(row < mine, 0, 1 + lax.rem(lax.div(rest, cap), outer - 1))
    expert = (level * plane + near_index).astype(wide)
    chosen = jnp.zeros((count, lanes), wide)
    share = jnp.zeros((count, lanes), wide)
    for k in range(topk):
        hit = ids[k:k + 1] == expert
        chosen = jnp.where(hit, 1.0, chosen)
        share = jnp.where(hit, shares[k:k + 1], share)
    older = lax.broadcasted_iota(jnp.int32, (lanes, lanes), 0)
    newer = lax.broadcasted_iota(jnp.int32, (lanes, lanes), 1)
    before = (older < newer) & (lax.div(older, toks) == lax.div(newer, toks))
    rank = jnp.dot(chosen.astype(low), jnp.where(before, 1.0, 0.0).astype(low), preferred_element_type=wide)
    slot = lax.rem(row, cap).astype(wide)
    own_step = lax.div(lane, toks) == row_step
    held = (chosen > 0.5) & own_step & (rank == slot)
    v.pick[...] = jnp.where(held, 1.0, 0.0).astype(low)
    flipped = jnp.where(held, share, 0.0).T
    high = flipped.astype(low)
    v.mix[:outer * toks] = high[:outer * toks]
    v.mix[outer * toks:] = (flipped - high.astype(wide)).astype(low)[:outer * toks]

    loads[2].wait()
    head_width = size.depth // local
    lane = lax.broadcasted_iota(jnp.int32, (local, size.depth), 1)
    row = lax.broadcasted_iota(jnp.int32, (local, size.depth), 0)
    own_head = lax.div(lane, head_width) == row
    begins = range(0, toks, half)
    order = [(step, begin) for step in (0, 1) for begin in begins]
    order += [(step, begin) for begin in begins for step in (2, 3)]
    for step, begin in order:
        span = pl.ds(begin, half)
        if step:
            settle(v.arrived.at[step, span], v.out_recv.at[begin // half, step])
        source = v.leaving[my_tp, span] if step == 0 else v.arrived[step, span]
        flat = source.reshape(half * local, latent)
        for column in range(0, size.depth, 256):
            product = jnp.dot(flat, v.up[:, column:column + 256], preferred_element_type=wide)
            product = product.reshape(half, local, 256)
            kept = jnp.where(own_head[None, :, column:column + 256], product, 0.0)
            value = jnp.sum(kept, axis=1).astype(low)
            v.heads[step * toks + begin:step * toks + begin + half, column:column + 256] = value
    loads[3].wait()

    def project(n):
        product = jnp.dot(v.heads[...], v.proj[:, n * tile:(n + 1) * tile], preferred_element_type=wide)
        v.total[n] = product[:toks]
        v.across[n] = product[2 * toks:3 * toks]
        v.partial[n, 0] = product[toks:2 * toks].astype(low)
        v.partial[n, 1] = product[3 * toks:].astype(low)
        remote(v.partial.at[n], v.parts.at[n], 2, v.pair_recv.at[n], {"tp": tp_peer[1]})

    def pass_on(n):
        settle(v.parts.at[n], v.pair_recv.at[n])
        v.total[n] += v.parts[n, 0].astype(wide)
        v.crossing[n] = (v.across[n] + v.parts[n, 1].astype(wide)).astype(low)
        remote(v.crossing.at[n], v.crossed.at[n], 3, v.part_recv.at[n], {"tp": tp_peer[2]})

    ahead = 3
    for n in range(tiles + ahead):
        if n < tiles:
            project(n)
        if n >= ahead:
            pass_on(n - ahead)
    line = outer == 4
    edge = (level == 0) | (level == outer - 1)

    def to_level(n, step):
        remote(v.block.at[n, pl.ds(0, toks)], v.block.at[n, pl.ds(step * toks, toks)], 4, v.far_recv.at[n, step % 2], far(step))

    def near_sends(out, into, kind, recv):
        for hop in range(1, plane):
            remote(out.at[near_peer[hop]], into.at[me], kind, recv, near(near_peer[hop]))

    def residual(n):
        settle(v.crossed.at[n], v.part_recv.at[n])
        value = v.total[n] + v.crossed[n].astype(wide)
        hidden = (v.hidden_in[:, n * tile:(n + 1) * tile].astype(wide) + value).astype(low)
        v.block[n, :toks] = hidden
        for step in range(1, outer):
            if line and step == 1:
                pl.when(level != outer - 1)(functools.partial(to_level, n, step))
            elif line and step == outer - 1:
                pl.when(level != 0)(functools.partial(to_level, n, step))
            else:
                to_level(n, step)
        picked = jnp.dot(v.pick[:mine, :toks], hidden, preferred_element_type=wide).astype(low)
        for index in range(plane):
            v.own_out[n, index] = picked[index * cap:(index + 1) * cap]
        near_sends(v.own_out.at[n], v.own_in.at[n], 5, v.near_recv.at[n, 0])
        v.own_in[n, me] = v.own_out[n, me]

    def relay(n):
        settle(v.block.at[n, pl.ds(0, (outer // 2 - (0 if outer % 2 else 1)) * toks)], v.far_recv.at[n, 0])
        if line:
            def pass_up():
                remote(
                    v.block.at[n, pl.ds(2 * toks, toks)], v.block.at[n, pl.ds(3 * toks, toks)], 4,
                    v.far_recv.at[n, 1], far(1),
                )

            def pass_down():
                remote(
                    v.block.at[n, pl.ds(2 * toks, toks)], v.block.at[n, pl.ds(toks, toks)], 4,
                    v.far_recv.at[n, 1], far(3),
                )

            pl.when(level == 2)(pass_up)
            pl.when(level == 1)(pass_down)

    def dispatch(n):
        settle(v.block.at[n, pl.ds(0, outer // 2 * toks)], v.far_recv.at[n, 1])
        picked = jnp.dot(
            v.pick[mine:, :outer * toks], v.block[n], preferred_element_type=wide
        ).astype(low)
        for index in range(plane):
            for step in range(outer - 1):
                first = (index * (outer - 1) + step) * cap
                v.far_out[n, index, step] = picked[first:first + cap]
        near_sends(v.far_out.at[n], v.far_in.at[n], 6, v.near_recv.at[n, 1])
        v.far_in[n, me] = v.far_out[n, me]

    def gather(own, distant, into):
        for index in range(plane):
            into[index * cap:(index + 1) * cap] = own[index]
            for step in range(outer - 1):
                first = mine + (index * (outer - 1) + step) * cap
                into[first:first + cap] = distant[index, step]

    def consume(n):
        settle(v.own_in.at[n, pl.ds(0, plane - 1)], v.near_recv.at[n, 0])
        settle(v.far_in.at[n, pl.ds(0, plane - 1)], v.near_recv.at[n, 1])
        into = v.rows.at[n % 2]
        gather(v.own_in.at[n], v.far_in.at[n], into)
        rows = into[...].astype(wide)
        square = rows * rows
        folded = square[:, :128]
        for first in range(128, tile, 128):
            folded = folded + square[:, first:first + 128]
        gain = v.gain[pl.ds(n * tile, tile)]
        scaled = (rows * gain[None, :]).astype(low)
        product = jnp.dot(scaled, v.gate[n * tile:(n + 1) * tile, :], preferred_element_type=wide)
        if n == 0:
            v.squares[...] = folded
            v.acc[...] = product
        else:
            v.squares[...] += folded
            v.acc[...] += product

    loads[4].wait()
    for n in range(tiles):
        residual(n)
    loads[5].wait()
    loads[6].wait()
    behind, lag = 0, 3
    for n in range(tiles + lag):
        if n < tiles:
            relay(n)
        if behind <= n < tiles + behind:
            dispatch(n - behind)
        if n >= lag:
            consume(n - lag)
    inv_norm = lax.rsqrt(jnp.sum(v.squares[...], axis=1, keepdims=True) / size.width + norm_eps)
    v.inner[...] = jax.nn.silu(v.acc[...] * inv_norm).astype(low)
    loads[7].wait()

    for n in range(tiles):
        answer = jnp.dot(v.inner[...], v.down[:, n * tile:(n + 1) * tile], preferred_element_type=wide).astype(low)
        for index in range(plane):
            v.own_answers[n, index] = answer[index * cap:(index + 1) * cap]
            for step in range(outer - 1):
                first = mine + (index * (outer - 1) + step) * cap
                v.far_answers[n, index, step] = answer[first:first + cap]
        near_sends(v.far_answers.at[n], v.far_back.at[n], 7, v.back_recv.at[n, 1])
        v.far_back[n, me] = v.far_answers[n, me]
    for n in range(tiles):
        near_sends(v.own_answers.at[n], v.own_back.at[n], 8, v.back_recv.at[n, 0])
        v.own_back[n, me] = v.own_answers[n, me]

    def combine(n):
        settle(v.far_back.at[n, pl.ds(0, plane - 1)], v.back_recv.at[n, 1])
        into = v.rows.at[n % 2]
        for index in range(plane):
            for step in range(outer - 1):
                first = mine + (index * (outer - 1) + step) * cap
                into[first:first + cap] = v.far_back[n, index, step]
        mixed = jnp.dot(v.mix[:, mine:], into[mine:], preferred_element_type=wide)
        mixed = mixed[:outer * toks] + mixed[outer * toks:]
        for step in sorted(range(1, outer), key=lambda step: step != 2):
            v.owed[n, step] = mixed[step * toks:(step + 1) * toks].astype(low)
            remote(v.owed.at[n, step], v.owing.at[n, step], 9, v.owed_recv.at[n], far(outer - step))

    def finish(n):
        settle(v.own_back.at[n, pl.ds(0, plane - 1)], v.back_recv.at[n, 0])
        into = v.rows.at[n % 2]
        for index in range(plane):
            into[index * cap:(index + 1) * cap] = v.own_back[n, index]
        mixed = jnp.dot(v.mix[:, :mine], into[:mine], preferred_element_type=wide)
        value = v.block[n, :toks].astype(wide) + mixed[:toks] + mixed[outer * toks:outer * toks + toks]
        settle(v.owing.at[n, pl.ds(1, outer - 1)], v.owed_recv.at[n])
        for step in range(1, outer):
            value = value + v.owing[n, step].astype(wide)
        out_ref[:, n * tile:(n + 1) * tile] = value.astype(low)

    for n in range(tiles):
        combine(n)
    for n in range(tiles):
        finish(n)
    others = pl.ds(0, plane - 1)
    for kind, like in enumerate((
        v.leaving.at[pl.ds(0, group - 1)], v.meta_in.at[pl.ds(0, outer - 1)], v.partial, v.crossing,
        None, v.own_out.at[:, others], v.far_out.at[:, others], v.far_answers.at[:, others],
        v.own_answers.at[:, others], v.owed.at[:, pl.ds(0, outer - 1)],
    )):
        if like is not None:
            settle(like, v.send_sem.at[kind])
    if line:
        pl.when(edge)(lambda: settle(v.block.at[:, pl.ds(0, 2 * toks)], v.send_sem.at[4]))
        pl.when(jnp.logical_not(edge))(lambda: settle(v.block, v.send_sem.at[4]))
    else:
        settle(v.block.at[:, pl.ds(0, (outer - 1) * toks)], v.send_sem.at[4])


def per_device(
    hidden_in,
    query_latent,
    query_rope,
    cache_latent,
    cache_rope,
    lengths,
    value_up,
    out_proj,
    norm_gain,
    expert_gate,
    expert_down,
    expert_ids,
    affinity,
):
    toks, head_count, latent = query_latent.shape
    dp, tp = lax.axis_size("dp"), lax.axis_size("tp")
    inner_dp = 2 if dp % 2 == 0 else 1
    outer, plane = dp // inner_dp, inner_dp * tp
    experts = expert_gate.shape[0] * dp * tp
    cap = max(2, -(-expert_ids.size // experts))
    width, ff = expert_gate.shape[1:]
    tile = 512 if width % 512 == 0 else 128
    topk = expert_ids.shape[1]
    batch = 2 if toks % 2 == 0 else 1
    spans = [(0, batch), (batch, toks - batch)]
    if toks % 8 == 0:
        spans = [(0, batch), (batch, 4 - batch), (4, 4), (8, toks - 8)]
    lanes = 128 * (-(-outer * toks // 128))
    size = types.SimpleNamespace(
        toks=toks, heads=head_count, latent=latent, context=cache_latent.shape[1], rope=cache_rope.shape[1],
        depth=out_proj.shape[0], width=width, ff=ff, group=tp, local=head_count // tp, tp=tp, inner_dp=inner_dp,
        outer=outer, plane=plane, cap=cap, count=plane * outer * cap, tile=tile,
        tiles=width // tile, batch=batch, spans=spans, halves=2 if toks % 4 == 0 else 1, topk=topk, lanes=lanes,
    )
    plan = scratch_plan(size)
    hbm = pl.BlockSpec(memory_space=pl.ANY)
    return pl.pallas_call(
        functools.partial(layer_kernel, size, tuple(plan)),
        out_shape=pltpu.VMEM((toks, width), low),
        in_specs=[hbm] * 13,
        out_specs=pl.BlockSpec(memory_space=pltpu.VMEM),
        scratch_shapes=list(plan.values()),
        compiler_params=pltpu.CompilerParams(
            collective_id=0, has_side_effects=True, vmem_limit_bytes=60 * 1024 * 1024
        ),
    )(
        query_latent, query_rope, cache_latent, cache_rope, lengths, hidden_in, norm_gain, value_up, out_proj,
        expert_ids.T, affinity.T, expert_gate, expert_down,
    )


def solution(mesh):
    spread = P(("dp", "tp"))
    return jax.shard_map(
        per_device,
        mesh=mesh,
        in_specs=(
            spread, spread, spread, spread, spread, spread, P(None, "tp"), P("tp", None), P(), spread, spread,
            spread, spread,
        ),
        out_specs=spread,
        check_vma=False,
    )
```
